32 devices in a mesh: seq: 8 (over y, x, core), tp: 4 (over z).
Axes of the slice: x: 2, y: 2, z: 4, core: 2. Of those that a mesh axis runs over, the one named last changes fastest.
Arguments:
- queries: bfloat16 [1024, 4096], P('seq', 'tp'), may hold values from -16 to 16
- keyvalues: bfloat16 [2, 1024, 1024], P(None, 'seq', 'tp'), may hold values from -16 to 16
- stretch_order: int32 [8], replicated, may hold values from 0 to 7, each once
- block_table: int32 [8, 8], replicated, may hold values 0 or 1
- proj_weight: bfloat16 [4096, 2048], P('tp'), may hold values from -0.09375 to 0.09375
Outputs:
- projected: bfloat16 [1024, 2048], P('seq', 'tp')
The draws below stay inside these ranges and needn't reach their ends.
Inputs may be any that keep to these rules, and one draw needn't show every extreme that they name: `stretch_order`: every stretch number 0 to 7 appears once. `block_table`: entry [i, j] matters only where j < i.
All inputs are finite; a program needn't handle non-finite values.
Results may differ from the reference program's by a relative error of at most 0.014.
Values may be sent and summed in bfloat16 or wider, within the bound.
A program may use at most 128 MiB of HBM per device.

```python
import jax
import jax.numpy as jnp
from jax import lax

QUERY_HEADS = 32
KEY_VALUE_HEADS = 8
HEAD_SIZE = 128
DOUT = 2048
STRETCH_TOKENS = 128
NCHUNK = 8
SEQUENCE_TOKENS = 1024


def query_key_pair(key):
    base = jax.random.fold_in(key, 11)
    random_seeds = jax.random.split(base, 3)
    queries = jnp.clip(jax.random.normal(random_seeds[0], (SEQUENCE_TOKENS, QUERY_HEADS * HEAD_SIZE), jnp.float32), -4.0, 4.0)
    key_matrix = jnp.clip(jax.random.normal(random_seeds[1], (SEQUENCE_TOKENS, KEY_VALUE_HEADS * HEAD_SIZE), jnp.float32), -4.0, 4.0)
    value_vectors = jnp.clip(jax.random.normal(random_seeds[2], (SEQUENCE_TOKENS, KEY_VALUE_HEADS * HEAD_SIZE), jnp.float32), -4.0, 4.0)
    return (queries, jnp.stack([key_matrix, value_vectors]))


def draw_queries(key, part):
    return query_key_pair(key)[0].astype(jnp.bfloat16)


def draw_keyvalues(key, part):
    return query_key_pair(key)[1].astype(jnp.bfloat16)


def set_ends(drawn, stream_key, low, top_value):
    longest = drawn.shape.index(max(drawn.shape))
    spots = []
    for shift in (0, 1):
        where = [jax.random.randint(jax.random.fold_in(stream_key, axis), (), 0, length) for axis, length in enumerate(drawn.shape)]
        where[longest] = (where[longest] + shift) % drawn.shape[longest]
        spots.append(tuple(where))
    return drawn.at[spots[0]].set(low).at[spots[1]].set(top_value)


def level_of(key, extent, cuts, low, top_value):
    factor_of = 1.0
    for dim, parts in cuts:
        steps = jax.random.uniform(jax.random.fold_in(jax.random.fold_in(key, 6), dim), (parts,), jnp.float32, low / len(cuts), top_value / len(cuts))
        factor_of = factor_of * jnp.repeat(jnp.exp(steps), extent[dim] // parts).reshape((-1,) + (1,) * (len(extent) - 1 - dim))
    return factor_of


def scatter_about(rng, dims, width, limit, pieces=(), kind=jnp.bfloat16):
    values = jax.random.normal(rng, dims, jnp.float32) * width
    if len(pieces) > 0:
        values = level_of(rng, dims, pieces, -0.22, 0.18) * values
    return jnp.clip(values, min=-limit, max=limit).astype(kind)


def setup_inputs(seed: int = 0) -> dict:
    key_of = jax.random.split(jax.random.key(seed), 6)
    queries = draw_queries(jax.random.fold_in(key_of[5], 71), 0)
    keyvalues = draw_keyvalues(jax.random.fold_in(key_of[5], 71), 0)
    stretch_order = jax.random.permutation(key_of[2], NCHUNK).astype(jnp.int32)
    block_table = set_ends((jax.random.randint(key_of[3], (NCHUNK, NCHUNK), 0, 4) < 3).astype(jnp.int32), jax.random.fold_in(key_of[3], 1), 0, 1)
    proj_weight = scatter_about(key_of[4], (QUERY_HEADS * HEAD_SIZE, DOUT), (QUERY_HEADS * HEAD_SIZE) ** -0.5, 0.09375, ((0, 4),))
    return {"queries": queries, "keyvalues": keyvalues, "stretch_order": stretch_order, "block_table": block_table, "proj_weight": proj_weight}


def reference(queries, keyvalues, stretch_order, block_table, proj_weight):
    row_index = jnp.arange(SEQUENCE_TOKENS, dtype=jnp.int32)
    row_stretch = stretch_order[row_index // STRETCH_TOKENS].astype(jnp.int32)
    row_pos = row_stretch * STRETCH_TOKENS + row_index % STRETCH_TOKENS
    group_width = QUERY_HEADS // KEY_VALUE_HEADS
    score_scale = 1.0 / (HEAD_SIZE ** 0.5)
    key_matrix = keyvalues[0].astype(jnp.float32).reshape(SEQUENCE_TOKENS, KEY_VALUE_HEADS, HEAD_SIZE)
    value_matrix = keyvalues[1].astype(jnp.float32).reshape(SEQUENCE_TOKENS, KEY_VALUE_HEADS, HEAD_SIZE)

    def block_out(block_index):
        start = (block_index * STRETCH_TOKENS).astype(jnp.int32)
        query_tile = lax.dynamic_slice_in_dim(queries, start, STRETCH_TOKENS, 0).astype(jnp.float32)
        query_tile = query_tile.reshape(STRETCH_TOKENS, KEY_VALUE_HEADS, group_width, HEAD_SIZE)
        query_stretch = lax.dynamic_slice_in_dim(row_stretch, start, STRETCH_TOKENS, 0)
        query_pos = lax.dynamic_slice_in_dim(row_pos, start, STRETCH_TOKENS, 0)
        table_row = block_table[query_stretch[0]]
        table_hits = table_row[row_stretch]
        same_stretch = (row_stretch[None, :] == query_stretch[:, None]) & (row_pos[None, :] <= query_pos[:, None])
        earlier = (row_stretch[None, :] < query_stretch[:, None]) & (table_hits[None, :] == 1)
        allowed = same_stretch | earlier
        scores = jnp.einsum("tkgd,skd->kgts", query_tile, key_matrix) * score_scale
        scores = jnp.where(allowed, scores, -1e30)
        row_max = jnp.max(scores, axis=-1)
        weights = jnp.where(allowed, jnp.exp(scores - row_max[..., None]), 0.0)
        denominator = jnp.sum(weights, axis=-1)
        rounded = weights.astype(jnp.bfloat16).astype(jnp.float32)
        numerator = jnp.einsum("kgts,skd->kgtd", rounded, value_matrix)
        attended = numerator / denominator[..., None]
        attended = jnp.transpose(attended, (2, 0, 1, 3)).reshape(STRETCH_TOKENS, QUERY_HEADS * HEAD_SIZE)
        return attended.astype(jnp.bfloat16)

    blocks = lax.map(block_out, jnp.arange(NCHUNK, dtype=jnp.int32))
    attention = blocks.reshape(SEQUENCE_TOKENS, QUERY_HEADS * HEAD_SIZE)
    return jnp.dot(attention, proj_weight, preferred_element_type=jnp.float32).astype(jnp.bfloat16)
```

```python
import functools

import jax
import jax.numpy as jnp
from jax import lax
from jax.experimental import pallas as pl
from jax.experimental.pallas import tpu as pltpu
from jax.sharding import PartitionSpec as P

HEAD = 128
MASKED = -1e30
LOG2E = 1.4426950408889634
MESH = pl.DeviceIdType.MESH


def kernel(
    n, tp, q_hbm, kv_hbm, order_hbm, table_hbm, w_hbm, out_ref,
    order, table, q_in, q_rows, k_buf, v_buf, w_buf, run_max, acc, att, parts, got, relay,
    in_sem, k_send, v_send, k_recv, v_recv, k_fwd, v_fwd, p_send, p_recv, r_recv,
):
    rows = q_in.shape[0]
    kv_heads = k_buf.shape[1] // HEAD
    q_heads = q_in.shape[1] // HEAD
    group = q_heads // kv_heads
    grows = group * rows
    width = got.shape[2]
    chips = n // 2
    me = lax.axis_index("seq")
    mt = lax.axis_index("tp")
    chip = me // 2
    core = me % 2
    partner = chip * 2 + 1 - core

    def slot(ref, s, count=1):
        return ref.at[pl.ds(pl.multiple_of(s * rows, rows), count * rows)]

    own_k = pltpu.make_async_copy(kv_hbm.at[0], slot(k_buf, me), in_sem.at[0])
    own_v = pltpu.make_async_copy(kv_hbm.at[1], slot(v_buf, me), in_sem.at[1])
    load_q = pltpu.make_async_copy(q_hbm, q_in, in_sem.at[2])
    load_w = pltpu.make_async_copy(w_hbm, w_buf, in_sem.at[3])
    own_k.start()
    own_v.start()
    load_q.start()
    load_order = pltpu.make_async_copy(order_hbm, order, in_sem.at[4])
    load_table = pltpu.make_async_copy(table_hbm, table, in_sem.at[5])
    load_order.start()
    load_table.start()
    load_w.start()

    barrier = pltpu.get_barrier_semaphore()

    def peer(j):
        return ((chip + j) % chips) * 2 + core

    def each(lo, hi, body):
        if hi - lo <= 8:
            for j in range(lo, hi):
                body(j)
        else:
            lax.fori_loop(lo, hi, lambda j, c: (body(j), c)[1], 0)

    def greet_seq(s):
        pl.semaphore_signal(barrier, inc=1, device_id={"seq": s}, device_id_type=MESH)

    def greet_tp(t):
        pl.semaphore_signal(barrier, inc=1, device_id={"tp": t}, device_id_type=MESH)

    square = chips == 4
    chip_x, chip_y = chip % 2, chip // 2
    xn = (chip_y * 2 + 1 - chip_x) * 2 + 1 - core
    yn = ((1 - chip_y) * 2 + chip_x) * 2 + 1 - core
    dn = ((1 - chip_y) * 2 + 1 - chip_x) * 2 + core
    line = tp == 4
    side = mt // 2
    inner = mt % 2 * (1 - side) + (1 - mt % 2) * side

    def mirror(d):
        return d * (1 - side) + (3 - d) * side

    greet_seq(partner)
    if square:
        greet_seq(xn)
        greet_seq(yn)
        seq_peers = 3
    else:
        each(1, chips, lambda j: greet_seq(peer(j)))
        seq_peers = chips
    if line:
        greet_tp(mirror(2))
        greet_tp(mirror(1 - inner))

        @pl.when(inner == 1)
        def _():
            greet_tp(mirror(3))

        tp_peers = 2 + inner
    else:
        for j in range(1, tp):
            greet_tp((mt + j) % tp)
        tp_peers = tp - 1

    own_k.wait()
    own_v.wait()
    pl.semaphore_wait(barrier, seq_peers + tp_peers)

    def remote(buf, s, send, recv, index, target):
        return pltpu.make_async_remote_copy(
            src_ref=slot(buf, s), dst_ref=slot(buf, s),
            send_sem=send.at[index], recv_sem=recv.at[s],
            device_id={"seq": target}, device_id_type=MESH,
        )

    def send_all(j):
        remote(k_buf, me, k_send, k_recv, j, peer(j)).start()
        remote(v_buf, me, v_send, v_recv, j, peer(j)).start()

    remote(k_buf, me, k_fwd, k_recv, 0, partner).start()
    remote(v_buf, me, v_fwd, v_recv, 0, partner).start()
    if square:
        remote(k_buf, me, k_send, k_recv, 0, xn).start()
        remote(v_buf, me, v_send, v_recv, 0, yn).start()
        remote(v_buf, me, v_send, v_recv, 1, xn).start()
        remote(k_buf, me, k_send, k_recv, 1, yn).start()
    else:
        each(1, chips, send_all)

    load_q.wait()
    for h in range(q_heads):
        q_rows[h * rows:(h + 1) * rows, :] = q_in[:, h * HEAD:(h + 1) * HEAD]

    def bias_of(s):
        key_stretch = order[s]
        seen = jnp.logical_and(key_stretch < my_stretch, table[my_stretch, key_stretch] == 1)
        return jnp.where(seen, 0.0, MASKED).astype(jnp.float32)

    load_order.wait()
    load_table.wait()
    my_stretch = order[me]
    scale = LOG2E / HEAD**0.5

    def attend(slots, first=False):
        count = len(slots)

        def rows_of(buf, cols):
            return jnp.concatenate(
                [buf[pl.ds(pl.multiple_of(s * rows, rows), rows), cols] for s in slots], axis=0
            )

        bias = jnp.concatenate(
            [jnp.full((1, rows), bias_of(s), jnp.float32) for s in slots], axis=1
        )
        for g in range(kv_heads):
            cols = slice(g * HEAD, (g + 1) * HEAD)
            here = slice(g * grows, (g + 1) * grows)
            keys = rows_of(k_buf, cols)
            values = rows_of(v_buf, cols)
            scores = lax.dot_general(
                q_rows[here, :], keys, (((1,), (1,)), ((), ())),
                preferred_element_type=jnp.float32,
            )
            if first:
                shape = (grows, count * rows)
                q_pos = lax.broadcasted_iota(jnp.int32, shape, 0) % rows
                k_pos = lax.broadcasted_iota(jnp.int32, shape, 1)
                scores = jnp.where(
                    k_pos < rows, jnp.where(k_pos <= q_pos, scores, MASKED), scores + bias
                )
            else:
                scores = scores + bias
            top = jnp.max(scores, axis=1, keepdims=True)
            if first:
                new_max = top
            else:
                old_max = run_max[here, 0:1]
                new_max = jnp.maximum(old_max, top)
            weights = jnp.exp2((scores - new_max) * scale).astype(jnp.bfloat16)
            wide = jnp.concatenate([values, jnp.ones_like(values)], axis=1)
            added = jnp.dot(weights, wide, preferred_element_type=jnp.float32)
            if first:
                acc[here, :] = added
            else:
                acc[here, :] = acc[here, :] * jnp.exp2((old_max - new_max) * scale) + added
            run_max[here, :] = jnp.broadcast_to(new_max, (grows, HEAD))

    def wait_slot(s):
        remote(k_buf, s, k_fwd, k_recv, 0, partner).wait_recv()
        remote(v_buf, s, v_fwd, v_recv, 0, partner).wait_recv()

    wait_slot(partner)
    attend([me, partner], True)

    def step(j):
        s = ((chip - j + chips) % chips) * 2 + core
        other = ((chip - j + chips) % chips) * 2 + 1 - core
        remote(k_buf, s, k_fwd, k_recv, j, partner).wait_recv()
        remote(k_buf, s, k_fwd, k_recv, j, partner).start()
        remote(v_buf, s, v_fwd, v_recv, j, partner).wait_recv()
        remote(v_buf, s, v_fwd, v_recv, j, partner).start()
        wait_slot(other)
        attend([s, other])

    def arrive(buf, recv, fwd, s, j, onward=None, send=None):
        remote(buf, s, fwd, recv, j, partner).wait_recv()
        if onward is not None:
            remote(buf, s, send, recv, 2, onward).start()
        remote(buf, s, fwd, recv, j, partner).start()

    if square:
        arrive(k_buf, k_recv, k_fwd, xn, 1, yn, k_send)
        arrive(v_buf, v_recv, v_fwd, yn, 2, xn, v_send)
        arrive(v_buf, v_recv, v_fwd, xn, 1)
        arrive(k_buf, k_recv, k_fwd, yn, 2)
        attend([xn, yn])
        arrive(k_buf, k_recv, k_fwd, dn, 3)
        arrive(v_buf, v_recv, v_fwd, dn, 3)
        xo, yo, do = xn - 1 + 2 * core, yn - 1 + 2 * core, dn + 1 - 2 * core
        wait_slot(xo)
        wait_slot(yo)
        attend([xo, yo, dn])
        wait_slot(do)
        attend([do])
    else:
        each(1, chips, step)

    for h in range(q_heads):
        here = slice(h * rows, (h + 1) * rows)
        att[:, h * HEAD:(h + 1) * HEAD] = (
            acc[here, :HEAD] / acc[here, HEAD:]
        ).astype(jnp.bfloat16)

    load_w.wait()

    def project(t):
        return jnp.dot(
            att[...], w_buf[:, pl.ds(pl.multiple_of(t * width, width), width)],
            preferred_element_type=jnp.float32,
        )

    def part_copy(j, source, target):
        return pltpu.make_async_remote_copy(
            src_ref=parts.at[j], dst_ref=got.at[source],
            send_sem=p_send.at[j], recv_sem=p_recv.at[source],
            device_id={"tp": target}, device_id_type=MESH,
        )

    def piece_copy(i, dst, recv, target):
        piece = pl.ds(i * (rows // 4), rows // 4)
        return pltpu.make_async_remote_copy(
            src_ref=parts.at[2, piece], dst_ref=dst.at[piece],
            send_sem=p_send.at[2 + i], recv_sem=recv,
            device_id={"tp": target}, device_id_type=MESH,
        )

    if line:
        m0, m1, m2, m3 = (mirror(d) for d in range(4))

        @pl.when(inner == 0)
        def _():
            parts[2] = project(m3).astype(jnp.bfloat16)
            for i in range(4):
                piece_copy(i, relay, r_recv.at[i], m1).start()
            parts[0] = project(m2).astype(jnp.bfloat16)
            part_copy(0, mt, m2).start()
            parts[1] = project(m1).astype(jnp.bfloat16)
            part_copy(1, mt, m1).start()
            total = project(mt)
            part_copy(0, m1, m1).wait_recv()
            total = total + got[m1].astype(jnp.float32)
            for i in range(4):
                piece_copy(i, got.at[m2], r_recv.at[i], m2).wait_recv()
            total = total + got[m2].astype(jnp.float32)
            out_ref[...] = total.astype(out_ref.dtype)

        @pl.when(inner == 1)
        def _():
            parts[0] = project(m2).astype(jnp.bfloat16)
            part_copy(0, mt, m2).start()
            parts[1] = project(m0).astype(jnp.bfloat16)
            part_copy(1, mt, m0).start()
            far = project(m3)
            total = project(mt)
            for i in range(4):
                piece = slice(i * (rows // 4), (i + 1) * (rows // 4))
                piece_copy(i, relay, r_recv.at[i], m0).wait_recv()
                parts[2, piece] = (far[piece] + relay[piece].astype(jnp.float32)).astype(jnp.bfloat16)
                piece_copy(i, got.at[mt], r_recv.at[i], m3).start()
            for source in (m2, m3, m0):
                part_copy(0, source, source).wait_recv()
                total = total + got[source].astype(jnp.float32)
            out_ref[...] = total.astype(out_ref.dtype)

        part_copy(0, mt, m2).wait_send()
        part_copy(1, mt, m0).wait_send()
        for i in range(4):
            piece_copy(i, relay, r_recv.at[i], m1).wait_send()
    else:
        ahead = sorted(range(1, tp), key=lambda j: -min(j, tp - j))
        for j in ahead:
            t = (mt + j) % tp
            parts[j] = project(t).astype(jnp.bfloat16)
            part_copy(j, mt, t).start()
        total = project(mt)
        for j in reversed(ahead):
            source = (mt + j) % tp
            part_copy(j, source, source).wait_recv()
            total = total + got[source].astype(jnp.float32)
        out_ref[...] = total.astype(out_ref.dtype)
        for j in ahead:
            part_copy(j, mt, (mt + j) % tp).wait_send()

    def drain(j):
        remote(k_buf, me, k_send, k_recv, j, peer(j)).wait_send()
        remote(v_buf, me, v_send, v_recv, j, peer(j)).wait_send()

    def drain_fwd(j):
        remote(k_buf, me, k_fwd, k_recv, j, partner).wait_send()
        remote(v_buf, me, v_fwd, v_recv, j, partner).wait_send()

    if square:
        for j in range(3):
            remote(k_buf, me, k_send, k_recv, j, yn).wait_send()
            remote(v_buf, me, v_send, v_recv, j, xn).wait_send()
    else:
        each(1, chips, drain)
    each(0, chips, drain_fwd)


def solution(mesh):
    n, tp = mesh.shape["seq"], mesh.shape["tp"]

    def per_device(queries, keyvalues, stretch_order, block_table, proj_weight):
        rows, q_width = queries.shape
        kv_width = keyvalues.shape[2]
        dout = proj_weight.shape[1]
        q_heads = q_width // HEAD
        dma = pltpu.SemaphoreType.DMA
        return pl.pallas_call(
            functools.partial(kernel, n, tp),
            out_shape=pltpu.VMEM((rows, dout // tp), jnp.bfloat16),
            in_specs=[
                pl.BlockSpec(memory_space=pl.ANY),
                pl.BlockSpec(memory_space=pl.ANY),
                pl.BlockSpec(memory_space=pl.ANY),
                pl.BlockSpec(memory_space=pl.ANY),
                pl.BlockSpec(memory_space=pl.ANY),
            ],
            out_specs=pl.BlockSpec(memory_space=pltpu.VMEM),
            scratch_shapes=[
                pltpu.SMEM(stretch_order.shape, jnp.int32),
                pltpu.SMEM(block_table.shape, jnp.int32),
                pltpu.VMEM((rows, q_width), jnp.bfloat16),
                pltpu.VMEM((q_heads * rows, HEAD), jnp.bfloat16),
                pltpu.VMEM((n * rows, kv_width), jnp.bfloat16),
                pltpu.VMEM((n * rows, kv_width), jnp.bfloat16),
                pltpu.VMEM(proj_weight.shape, jnp.bfloat16),
                pltpu.VMEM((q_heads * rows, HEAD), jnp.float32),
                pltpu.VMEM((q_heads * rows, 2 * HEAD), jnp.float32),
                pltpu.VMEM((rows, q_width), jnp.bfloat16),
                pltpu.VMEM((tp, rows, dout // tp), jnp.bfloat16),
                pltpu.VMEM((tp, rows, dout // tp), jnp.bfloat16),
                pltpu.VMEM((rows, dout // tp), jnp.bfloat16),
                dma((6,)),
                dma((n // 2,)), dma((n // 2,)),
                dma((n,)), dma((n,)),
                dma((n // 2,)), dma((n // 2,)),
                dma((max(tp, 6),)), dma((tp,)), dma((4,)),
            ],
            compiler_params=pltpu.CompilerParams(
                collective_id=0, has_side_effects=True, vmem_limit_bytes=48 << 20,
            ),
        )(*(pltpu.with_memory_space_constraint(a, pltpu.HBM)
            for a in (queries, keyvalues, stretch_order, block_table, proj_weight)))

    return jax.shard_map(
        per_device, mesh=mesh,
        in_specs=(P("seq", "tp"), P(None, "seq", "tp"), P(), P(), P("tp", None)),
        out_specs=P("seq", "tp"), check_vma=False,
    )
```

```python
import functools

import jax
import jax.numpy as jnp
from jax import lax
from jax.experimental import pallas as pl
from jax.experimental.pallas import tpu as pltpu
from jax.sharding import PartitionSpec as P

HEAD = 128
MASKED = -1e30
LOG2E = 1.4426950408889634
MESH = pl.DeviceIdType.MESH
F32 = jnp.float32
BF16 = jnp.bfloat16


def kernel(
    n, tp, q_hbm, kv_hbm, order_hbm, table_hbm, w_hbm, out_ref,
    order, table, q_in, q_t, k_buf, v_buf, w_buf, top_ref, acc, den, att, mine, parts, relay, got,
    in_sem, kv_send, k_recv, v_recv, p_send, r_recv, g_recv,
):
    rows = q_in.shape[0]
    kv_heads = k_buf.shape[1]
    q_heads = q_in.shape[1] // HEAD
    group = q_heads // kv_heads
    width = out_ref.shape[1]
    blocks, _, pcols = parts.shape[1:]
    half = rows // 2
    chips = n // 2
    me = lax.axis_index("seq")
    mt = lax.axis_index("tp")
    chip = me // 2
    core = me % 2
    partner = chip * 2 + 1 - core
    heads = range(kv_heads)

    own = []
    for g in heads:
        cols = slice(g * HEAD, (g + 1) * HEAD)
        own.append(pltpu.make_async_copy(kv_hbm.at[0, :, cols], k_buf.at[me, g], in_sem.at[4 + 2 * g]))
        own.append(pltpu.make_async_copy(kv_hbm.at[1, :, cols], v_buf.at[me, g], in_sem.at[5 + 2 * g]))
    load_q = pltpu.make_async_copy(q_hbm, q_in, in_sem.at[0])
    load_w = pltpu.make_async_copy(w_hbm, w_buf, in_sem.at[1])
    load_order = pltpu.make_async_copy(order_hbm, order, in_sem.at[2])
    load_table = pltpu.make_async_copy(table_hbm, table, in_sem.at[3])
    for c in own:
        c.start()
    load_q.start()
    load_order.start()
    load_table.start()
    load_w.start()

    barrier = pltpu.get_barrier_semaphore()

    def peer(j):
        return ((chip + j) % chips) * 2 + core

    def each(lo, hi, body):
        if hi - lo <= 8:
            for j in range(lo, hi):
                body(j)
        else:
            lax.fori_loop(lo, hi, lambda j, c: (body(j), c)[1], 0)

    def greet_seq(s):
        pl.semaphore_signal(barrier, inc=1, device_id={"seq": s}, device_id_type=MESH)

    def greet_tp(t):
        pl.semaphore_signal(barrier, inc=1, device_id={"tp": t}, device_id_type=MESH)

    square = chips == 4
    chip_x, chip_y = chip % 2, chip // 2
    x0 = (chip_y * 2 + 1 - chip_x) * 2
    y0 = ((1 - chip_y) * 2 + chip_x) * 2
    d0 = ((1 - chip_y) * 2 + 1 - chip_x) * 2
    x1, y1, d1 = x0 + 1, y0 + 1, d0 + 1
    line = tp == 4
    side = mt // 2
    inner = mt % 2 * (1 - side) + (1 - mt % 2) * side

    def mirror(d):
        return d * (1 - side) + (3 - d) * side

    greet_seq(partner)
    if square:
        greet_seq(x1)
        greet_seq(y1)

        @pl.when(core == 1)
        def _():
            greet_seq(x0)
            greet_seq(y0)

        seq_peers = 3 + 2 * core
    else:
        each(1, chips, lambda j: greet_seq(peer(j)))
        seq_peers = chips
    if line:
        greet_tp(mirror(2))
        greet_tp(mirror(1 - inner))

        @pl.when(inner == 1)
        def _():
            greet_tp(mirror(3))

        tp_peers = 2 + inner
    else:
        for j in range(1, tp):
            greet_tp((mt + j) % tp)
        tp_peers = tp - 1

    for c in own:
        c.wait()
    pl.semaphore_wait(barrier, seq_peers + tp_peers)

    def piece(buf, recv, s, g, index, target):
        return pltpu.make_async_remote_copy(
            src_ref=buf.at[s, g], dst_ref=buf.at[s, g],
            send_sem=kv_send.at[index], recv_sem=recv.at[s, g],
            device_id={"seq": target}, device_id_type=MESH,
        )

    def k_piece(s, g, index, target):
        return piece(k_buf, k_recv, s, g, index, target)

    def v_piece(s, g, index, target):
        return piece(v_buf, v_recv, s, g, index, target)

    base = 4 * kv_heads
    mark = 2 * kv_heads
    if square:
        for g in heads:
            k_piece(me, g, g, x1).start()
            v_piece(me, g, mark + g, y1).start()
            k_piece(me, g, base + g, partner).start()
            v_piece(me, g, base + kv_heads + g, partner).start()
        for g in heads:
            v_piece(me, g, kv_heads + g, x1).start()
            k_piece(me, g, mark + kv_heads + g, y1).start()
        base += mark
    else:
        def send_all(j, target):
            for g in heads:
                k_piece(me, g, j * mark + g, target).start()
                v_piece(me, g, j * mark + kv_heads + g, target).start()

        send_all(0, partner)
        each(1, chips, lambda j: send_all(j, peer(j)))
        base = mark * chips

    load_q.wait()
    for g in heads:
        for j in range(group):
            h = g * group + j
            q_t[g, :, j * rows:(j + 1) * rows] = q_in[:, h * HEAD:(h + 1) * HEAD].T

    load_order.wait()
    load_table.wait()
    my_stretch = order[me]
    scale = LOG2E / HEAD**0.5

    def bias_of(s):
        key_stretch = order[s]
        seen = jnp.logical_and(key_stretch < my_stretch, table[my_stretch, key_stretch] == 1)
        return jnp.where(seen, 0.0, MASKED).astype(F32)

    def attend(g, slots, first=False):
        queries = q_t[g]
        scores, tops, biases = [], [], []
        for i, s in enumerate(slots):
            part = jnp.dot(k_buf[s, g], queries, preferred_element_type=F32)
            if first and i == 0:
                k_pos = lax.broadcasted_iota(jnp.int32, part.shape, 0)
                q_pos = lax.broadcasted_iota(jnp.int32, part.shape, 1) % rows
                part = jnp.where(k_pos <= q_pos, part, MASKED)
                bias = 0.0
            else:
                bias = bias_of(s)
            scores.append(part)
            biases.append(bias)
            tops.append(jnp.max(part, axis=0, keepdims=True) + bias)
        new_top = functools.reduce(jnp.maximum, tops)
        if not first:
            old_top = top_ref[g]
            new_top = jnp.maximum(new_top, old_top)
        weights = jnp.concatenate(
            [jnp.exp2((p - (new_top - b)) * scale).astype(BF16) for p, b in zip(scores, biases)], axis=0
        )
        values = jnp.concatenate([v_buf[s, g] for s in slots], axis=0).T
        tall = jnp.concatenate([values, jnp.ones((16, values.shape[1]), BF16)], axis=0)
        added = jnp.dot(tall, weights, preferred_element_type=F32)
        if first:
            acc[g] = added[:HEAD]
            den[g] = added[HEAD:HEAD + 8]
        else:
            fade = jnp.exp2((old_top - new_top) * scale)
            acc[g] = acc[g] * fade + added[:HEAD]
            den[g] = den[g] * fade + added[HEAD:HEAD + 8]
        top_ref[g] = new_top

    def wait_slot(s, g):
        k_piece(s, g, 0, partner).wait_recv()
        v_piece(s, g, 0, partner).wait_recv()

    for g in heads:
        wait_slot(partner, g)
    for g in heads:
        attend(g, [me, partner], True)

    if square:
        near = [x1, y1, x0, y0]

        def hand_on(make, s, g, index, target=None, mark=0):
            make(s, g, 0, partner).wait_recv()
            if target is not None:
                make(s, g, mark, target).start()
            make(s, g, index, partner).start()

        relays = base
        hops = base + 4 * kv_heads

        @pl.when(core == 1)
        def _():
            i = 0
            for g in heads:
                for sx, sy in ((x1, y1), (x0, y0)):
                    hand_on(k_piece, sx, g, hops + i, y0, relays + i)
                    hand_on(v_piece, sy, g, hops + i + 1, x0, relays + i + 1)
                    i += 2

        for g in heads:
            @pl.when(core == 1)
            def _(g=g):
                i = hops + (kv_heads + g) * 4
                for sx, sy in ((x1, y1), (x0, y0)):
                    hand_on(v_piece, sx, g, i)
                    hand_on(k_piece, sy, g, i + 1)
                    i += 2

            @pl.when(core == 0)
            def _(g=g):
                for s in near:
                    wait_slot(s, g)

            attend(g, near)

            @pl.when(core == 0)
            def _(g=g):
                i = relays + g * 4
                for s in (d1, d0):
                    hand_on(k_piece, s, g, i)
                    hand_on(v_piece, s, g, i + 1)
                    i += 2

        for g in heads:
            @pl.when(core == 1)
            def _(g=g):
                wait_slot(d1, g)
                wait_slot(d0, g)

            attend(g, [d1, d0])
    else:
        def step(j):
            s = ((chip - j + chips) % chips) * 2 + core
            other = ((chip - j + chips) % chips) * 2 + 1 - core
            for g in heads:
                k_piece(s, g, 0, partner).wait_recv()
                k_piece(s, g, base + (j - 1) * mark + g, partner).start()
                v_piece(s, g, 0, partner).wait_recv()
                v_piece(s, g, base + (j - 1) * mark + kv_heads + g, partner).start()
            for g in heads:
                wait_slot(other, g)
            for g in heads:
                attend(g, [s, other])

        each(1, chips, step)

    for g in heads:
        share = 1.0 / den[g][0:1]
        for j in range(group):
            h = g * group + j
            cols = slice(j * rows, (j + 1) * rows)
            att[:, h * HEAD:(h + 1) * HEAD] = (acc[g, :, cols] * share[:, cols]).astype(BF16).T

    load_w.wait()

    def project(t, b):
        cols = pl.ds(pl.multiple_of(t * width + b * pcols, pcols), pcols)
        return jnp.dot(att[...], w_buf[:, cols], preferred_element_type=F32)

    def part_of(ref, slot, i):
        return ref.at[slot, i // 2, pl.ds(i % 2 * half, half)]

    def send_part(c, i, dst, slot, recv, target):
        return pltpu.make_async_remote_copy(
            src_ref=part_of(parts, c, i), dst_ref=part_of(dst, slot, i),
            send_sem=p_send.at[c, i], recv_sem=recv.at[slot, i],
            device_id={"tp": target}, device_id_type=MESH,
        )

    pieces = 2 * blocks
    if line:
        m0, m1, m2, m3 = (mirror(d) for d in range(4))

        def send_product(c, t, dst, slot, recv, target):
            for b in range(blocks):
                parts[c, b] = project(t, b).astype(BF16)
                for i in (2 * b, 2 * b + 1):
                    send_part(c, i, dst, slot, recv, target).start()

        @pl.when(inner == 0)
        def _():
            send_product(0, m3, relay, 0, r_recv, m1)
            send_product(1, m2, relay, 1, r_recv, m1)
            send_product(2, m1, got, 0, g_recv, m1)
            for b in range(blocks):
                mine[0, b] = project(mt, b)

        @pl.when(inner == 1)
        def _():
            send_product(2, m0, got, 0, g_recv, m0)
            for c, t in ((1, m3), (2, m2), (0, mt)):
                for b in range(blocks):
                    mine[c, b] = project(t, b)
            for c, target in ((0, m3), (1, m2)):
                for i in range(pieces):
                    b, r = i // 2, slice(i % 2 * half, (i % 2 + 1) * half)
                    send_part(2, i, relay, c, r_recv, m0).wait_recv()
                    parts[c, b, r] = (mine[1 + c, b, r] + relay[c, b, r].astype(F32)).astype(BF16)
                    send_part(c, i, got, 1, g_recv, target).start()

        for i in range(pieces):
            send_part(2, i, got, 0, g_recv, m0).wait_recv()
        for b in range(blocks):
            mine[0, b] = mine[0, b] + got[0, b].astype(F32)
        for i in range(pieces):
            b, r = i // 2, slice(i % 2 * half, (i % 2 + 1) * half)
            send_part(2, i, got, 1, g_recv, m0).wait_recv()
            out_ref[r, b * pcols:(b + 1) * pcols] = (mine[0, b, r] + got[1, b, r].astype(F32)).astype(BF16)
        for c in range(3):
            for i in range(pieces):
                send_part(c, i, got, 0, g_recv, m0).wait_send()
    else:
        ahead = sorted(range(1, tp), key=lambda j: -min(j, tp - j))
        for j in ahead:
            t = (mt + j) % tp
            for b in range(blocks):
                parts[j, b] = project(t, b).astype(BF16)
                for i in (2 * b, 2 * b + 1):
                    send_part(j, i, got, mt, g_recv, t).start()
        for b in range(blocks):
            mine[0, b] = project(mt, b)
        for j in reversed(ahead):
            source = (mt + j) % tp
            for i in range(pieces):
                send_part(j, i, got, source, g_recv, source).wait_recv()
            for b in range(blocks):
                mine[0, b] = mine[0, b] + got[source, b].astype(F32)
        for b in range(blocks):
            out_ref[:, b * pcols:(b + 1) * pcols] = mine[0, b].astype(BF16)
        for j in ahead:
            for i in range(pieces):
                send_part(j, i, got, mt, g_recv, mt).wait_send()

    def drain(i):
        k_piece(me, 0, i, partner).wait_send()

    if square:
        each(0, base, drain)
        each(base, base + 4 * kv_heads, drain)

        @pl.when(core == 1)
        def _():
            each(base + 4 * kv_heads, base + 12 * kv_heads, drain)
    else:
        each(0, 2 * base - mark, drain)


def solution(mesh):
    n, tp = mesh.shape["seq"], mesh.shape["tp"]

    def per_device(queries, keyvalues, stretch_order, block_table, proj_weight):
        rows, q_width = queries.shape
        kv_heads = keyvalues.shape[2] // HEAD
        width = proj_weight.shape[1] // tp
        pcols = 2 * HEAD if width % (2 * HEAD) == 0 else HEAD
        blocks = width // pcols
        group_rows = q_width // HEAD // kv_heads * rows
        line = tp == 4
        n_parts, n_got, n_mine = (3, 2, 3) if line else (tp, tp, 1)
        n_sends = 18 * kv_heads if n == 8 else 2 * kv_heads * n
        dma = pltpu.SemaphoreType.DMA
        args = (queries, keyvalues, stretch_order, block_table, proj_weight)
        return pl.pallas_call(
            functools.partial(kernel, n, tp),
            out_shape=pltpu.VMEM((rows, width), BF16),
            in_specs=[pl.BlockSpec(memory_space=pltpu.HBM)] * 5,
            out_specs=pl.BlockSpec(memory_space=pltpu.VMEM),
            scratch_shapes=[
                pltpu.SMEM(stretch_order.shape, jnp.int32),
                pltpu.SMEM(block_table.shape, jnp.int32),
                pltpu.VMEM((rows, q_width), BF16),
                pltpu.VMEM((kv_heads, HEAD, group_rows), BF16),
                pltpu.VMEM((n, kv_heads, rows, HEAD), BF16),
                pltpu.VMEM((n, kv_heads, rows, HEAD), BF16),
                pltpu.VMEM(proj_weight.shape, BF16),
                pltpu.VMEM((kv_heads, 1, group_rows), F32),
                pltpu.VMEM((kv_heads, HEAD, group_rows), F32),
                pltpu.VMEM((kv_heads, 8, group_rows), F32),
                pltpu.VMEM((rows, q_width), BF16),
                pltpu.VMEM((n_mine, blocks, rows, pcols), F32),
                pltpu.VMEM((n_parts, blocks, rows, pcols), BF16),
                pltpu.VMEM((2, blocks, rows, pcols), BF16),
                pltpu.VMEM((n_got, blocks, rows, pcols), BF16),
                dma((4 + 2 * kv_heads,)),
                dma((n_sends,)),
                dma((n, kv_heads)), dma((n, kv_heads)),
                dma((n_parts, 2 * blocks)), dma((2, 2 * blocks)), dma((n_got, 2 * blocks)),
            ],
            compiler_params=pltpu.CompilerParams(
                collective_id=0, has_side_effects=True, vmem_limit_bytes=48 << 20,
            ),
        )(*(pltpu.with_memory_space_constraint(a, pltpu.HBM) for a in args))

    return jax.shard_map(
        per_device, mesh=mesh,
        in_specs=(P("seq", "tp"), P(None, "seq", "tp"), P(), P(), P("tp", None)),
        out_specs=P("seq", "tp"), check_vma=False,
    )
```

```python
import functools

import jax
import jax.numpy as jnp
from jax import lax
from jax.experimental import pallas as pl
from jax.experimental.pallas import tpu as pltpu
from jax.sharding import PartitionSpec as P

HEAD = 128
MASKED = -1e30
LOG2E = 1.4426950408889634
MESH = pl.DeviceIdType.MESH
F32 = jnp.float32
BF16 = jnp.bfloat16


def kernel(
    n, tp, q_hbm, kv_hbm, order_hbm, table_hbm, w_hbm, out_ref,
    order, table, q_in, q_t, kv_buf, w_buf, top_ref, acc, den, att, mine, parts, relay, got,
    in_sem, kv_send, kv_recv, hop_recv, p_send, r_recv, g_recv, f_recv,
):
    rows = q_in.shape[0]
    kv_heads = kv_buf.shape[1]
    q_heads = q_in.shape[1] // HEAD
    group = q_heads // kv_heads
    width = out_ref.shape[1]
    blocks, _, pcols = parts.shape[1:]
    half = rows // 2
    chips = n // 2
    me = lax.axis_index("seq")
    mt = lax.axis_index("tp")
    chip = me // 2
    core = me % 2
    partner = chip * 2 + 1 - core
    heads = range(kv_heads)

    own = [
        pltpu.make_async_copy(
            kv_hbm.at[i, :, slice(g * HEAD, (g + 1) * HEAD)], kv_buf.at[me, g, i], in_sem.at[4]
        )
        for g in heads for i in range(2)
    ]
    load_q = pltpu.make_async_copy(q_hbm, q_in, in_sem.at[0])
    load_w = pltpu.make_async_copy(w_hbm, w_buf, in_sem.at[1])
    load_order = pltpu.make_async_copy(order_hbm, order, in_sem.at[2])
    load_table = pltpu.make_async_copy(table_hbm, table, in_sem.at[3])
    for c in own:
        c.start()
    load_q.start()
    load_order.start()
    load_table.start()
    load_w.start()

    barrier = pltpu.get_barrier_semaphore()

    def peer(j):
        return ((chip + j) % chips) * 2 + core

    def each(lo, hi, body):
        if hi - lo <= 8:
            for j in range(lo, hi):
                body(j)
        else:
            lax.fori_loop(lo, hi, lambda j, c: (body(j), c)[1], 0)

    def greet_seq(s):
        pl.semaphore_signal(barrier, inc=1, device_id={"seq": s}, device_id_type=MESH)

    def greet_tp(t):
        pl.semaphore_signal(barrier, inc=1, device_id={"tp": t}, device_id_type=MESH)

    square = chips == 4
    chip_x, chip_y = chip % 2, chip // 2
    x0 = (chip_y * 2 + 1 - chip_x) * 2
    y0 = ((1 - chip_y) * 2 + chip_x) * 2
    d0 = ((1 - chip_y) * 2 + 1 - chip_x) * 2
    x1, y1, d1 = x0 + 1, y0 + 1, d0 + 1
    line = tp == 4
    side = mt // 2
    inner = mt % 2 * (1 - side) + (1 - mt % 2) * side

    def mirror(d):
        return d * (1 - side) + (3 - d) * side

    greet_seq(partner)
    if square:
        greet_seq(x1)
        greet_seq(y1)

        @pl.when(core == 1)
        def _():
            greet_seq(x0)
            greet_seq(y0)

        seq_peers = 3 + 2 * core
    else:
        each(1, chips, lambda j: greet_seq(peer(j)))
        seq_peers = chips
    if line:
        greet_tp(mirror(2))
        greet_tp(mirror(1 - inner))

        @pl.when(inner == 1)
        def _():
            greet_tp(mirror(3))

        tp_peers = 2 + inner
    else:
        for j in range(1, tp):
            greet_tp((mt + j) % tp)
        tp_peers = tp - 1

    pltpu.make_async_copy(kv_buf.at[me], kv_buf.at[me], in_sem.at[4]).wait()
    pl.semaphore_wait(barrier, seq_peers + tp_peers)

    def copy(ref, recv_sem, target, turn=0):
        return pltpu.make_async_remote_copy(
            src_ref=ref, dst_ref=ref, send_sem=kv_send.at[turn], recv_sem=recv_sem,
            device_id={"seq": target}, device_id_type=MESH,
        )

    def slot(s, target):
        return copy(kv_buf.at[s], kv_recv.at[s], target)

    def near_sem(axis, c, g, i):
        return kv_recv.at[((axis * 2 + c) * kv_heads + g) * 2 + i]

    def far_sem(c, g, i):
        return kv_recv.at[(c * kv_heads + g) * 2 + i]

    def several(slots, recv_sem, turn=0):
        return copy(kv_buf.at[pl.ds(0, slots)], recv_sem, partner, turn)

    if square:
        for g in heads:
            for i in range(2):
                copy(kv_buf.at[me, g, i], hop_recv.at[0], partner).start()
        for i in range(2):
            for g in heads:
                copy(kv_buf.at[me, g, i], near_sem(0, core, g, i), x1).start()
                copy(kv_buf.at[me, g, 1 - i], near_sem(1, core, g, 1 - i), y1).start()
    else:
        slot(me, partner).start()
        each(1, chips, lambda j: slot(me, peer(j)).start())

    load_q.wait()
    for g in heads:
        for j in range(group):
            h = g * group + j
            q_t[g, :, j * rows:(j + 1) * rows] = q_in[:, h * HEAD:(h + 1) * HEAD].T

    load_order.wait()
    load_table.wait()
    my_stretch = order[me]
    scale = LOG2E / HEAD**0.5

    def bias_of(s):
        key_stretch = order[s]
        seen = jnp.logical_and(key_stretch < my_stretch, table[my_stretch, key_stretch] == 1)
        return jnp.where(seen, 0.0, MASKED).astype(F32)

    def attend(g, slots, first=False):
        queries = q_t[g]
        scores, tops, biases = [], [], []
        for i, s in enumerate(slots):
            part = jnp.dot(kv_buf[s, g, 0], queries, preferred_element_type=F32)
            if first and i == 0:
                k_pos = lax.broadcasted_iota(jnp.int32, part.shape, 0)
                q_pos = lax.broadcasted_iota(jnp.int32, part.shape, 1) % rows
                part = jnp.where(k_pos <= q_pos, part, MASKED)
                bias = 0.0
            else:
                bias = bias_of(s)
            scores.append(part)
            biases.append(bias)
            tops.append(jnp.max(part, axis=0, keepdims=True) + bias)
        new_top = functools.reduce(jnp.maximum, tops)
        if not first:
            old_top = top_ref[g]
            new_top = jnp.maximum(new_top, old_top)
        weights = jnp.concatenate(
            [jnp.exp2((p - (new_top - b)) * scale).astype(BF16) for p, b in zip(scores, biases)], axis=0
        )
        values = jnp.concatenate([kv_buf[s, g, 1] for s in slots], axis=0).T
        tall = jnp.concatenate([values, jnp.ones((16, values.shape[1]), BF16)], axis=0)
        added = jnp.dot(tall, weights, preferred_element_type=F32)
        if first:
            acc[g] = added[:HEAD]
            den[g] = added[HEAD:HEAD + 8]
        else:
            fade = jnp.exp2((old_top - new_top) * scale)
            acc[g] = acc[g] * fade + added[:HEAD]
            den[g] = den[g] * fade + added[HEAD:HEAD + 8]
        top_ref[g] = new_top

    if square:
        several(1, hop_recv.at[0]).wait_recv()
    else:
        slot(partner, partner).wait_recv()
    for g in heads:
        attend(g, [me, partner], True)

    if square:
        near, far = [x1, y1, x0, y0], [d1, d0]

        def arrive(s, g, i, sem, onward=None, onward_sem=None):
            ref = kv_buf.at[s, g, i]
            copy(ref, sem, partner).wait_recv()
            if onward is not None:
                copy(ref, onward_sem, onward, 1).start()
            copy(ref, hop_recv.at[1 + g], partner, 1).start()

        @pl.when(core == 1)
        def _():
            for g in heads:
                for c, sx, sy in ((1, x1, y1), (0, x0, y0)):
                    arrive(sx, g, 0, near_sem(0, c, g, 0), y0, far_sem(c, g, 0))
                    arrive(sy, g, 1, near_sem(1, c, g, 1), x0, far_sem(c, g, 1))
            for g in heads:
                for c, sx, sy in ((1, x1, y1), (0, x0, y0)):
                    arrive(sx, g, 1, near_sem(0, c, g, 1))
                    arrive(sy, g, 0, near_sem(1, c, g, 0))
                attend(g, near)
            for g in heads:
                several(1, hop_recv.at[1 + g]).wait_recv()
                attend(g, far)

        @pl.when(core == 0)
        def _():
            for g in heads:
                several(2, hop_recv.at[1 + g]).wait_recv()
                last = g == kv_heads - 1
                if not last:
                    attend(g, near)
                for c, s in ((1, d1), (0, d0)):
                    for i in range(2):
                        arrive(s, g, i, far_sem(c, g, i))
                attend(g, near + far if last else far)
    else:
        def step(j):
            s = ((chip - j + chips) % chips) * 2 + core
            other = ((chip - j + chips) % chips) * 2 + 1 - core
            slot(s, partner).wait_recv()
            slot(s, partner).start()
            slot(other, partner).wait_recv()
            for g in heads:
                attend(g, [s, other])

        each(1, chips, step)

    for g in heads:
        share = 1.0 / den[g][0:1]
        for j in range(group):
            h = g * group + j
            cols = slice(j * rows, (j + 1) * rows)
            att[:, h * HEAD:(h + 1) * HEAD] = (acc[g, :, cols] * share[:, cols]).astype(BF16).T

    load_w.wait()

    def project(t, b):
        cols = pl.ds(pl.multiple_of(t * width + b * pcols, pcols), pcols)
        return jnp.dot(att[...], w_buf[:, cols], preferred_element_type=F32)

    def part_of(ref, slot, i):
        return ref.at[slot, i // 2, pl.ds(i % 2 * half, half)]

    def send_part(c, i, dst, slot, recv_sem, target):
        return pltpu.make_async_remote_copy(
            src_ref=part_of(parts, c, i), dst_ref=part_of(dst, slot, i),
            send_sem=p_send.at[c], recv_sem=recv_sem,
            device_id={"tp": target}, device_id_type=MESH,
        )

    def whole_part(c, slot):
        return pltpu.make_async_remote_copy(
            src_ref=parts.at[c], dst_ref=got.at[slot], send_sem=p_send.at[c], recv_sem=g_recv.at[slot],
            device_id={"tp": mt}, device_id_type=MESH,
        )

    def drain():
        if square:
            several(3, hop_recv.at[0]).wait_send()

            @pl.when(core == 1)
            def _():
                several(6, hop_recv.at[0], 1).wait_send()

            @pl.when(core == 0)
            def _():
                several(2, hop_recv.at[0], 1).wait_send()
        else:
            several(n - 1, hop_recv.at[0]).wait_send()

    pieces = 2 * blocks
    if line:
        m0, m1, m2, m3 = (mirror(d) for d in range(4))

        def send_product(c, t, dst, slot, recv_sems, target):
            for b in range(blocks):
                parts[c, b] = project(t, b).astype(BF16)
                for i in (2 * b, 2 * b + 1):
                    send_part(c, i, dst, slot, recv_sems(i), target).start()

        def keep_own():
            for b in range(blocks):
                mine[0, b] = project(mt, b)

        @pl.when(inner == 0)
        def _():
            send_product(0, m3, relay, 0, lambda i: r_recv.at[0, i], m1)
            send_product(1, m2, relay, 1, lambda i: r_recv.at[1, i], m1)
            send_product(2, m1, got, 0, lambda i: g_recv.at[0], m1)
            keep_own()

        @pl.when(inner == 1)
        def _():
            send_product(2, m0, got, 0, lambda i: g_recv.at[0], m0)
            for c, t in ((1, m3), (2, m2), (0, mt)):
                for b in range(blocks):
                    mine[c, b] = project(t, b)
            for c, target in ((0, m3), (1, m2)):
                for i in range(pieces):
                    b, r = i // 2, slice(i % 2 * half, (i % 2 + 1) * half)
                    send_part(2, i, relay, c, r_recv.at[c, i], m0).wait_recv()
                    parts[c, b, r] = (mine[1 + c, b, r] + relay[c, b, r].astype(F32)).astype(BF16)
                    send_part(c, i, got, 1, f_recv.at[i], target).start()

        drain()
        whole_part(0, 0).wait_send()
        whole_part(2, 0).wait_recv()
        for b in range(blocks):
            mine[0, b] = mine[0, b] + got[0, b].astype(F32)
        whole_part(1 + inner, 0).wait_send()
        for i in range(pieces):
            b, r = i // 2, slice(i % 2 * half, (i % 2 + 1) * half)
            send_part(2, i, got, 1, f_recv.at[i], m0).wait_recv()
            out_ref[r, b * pcols:(b + 1) * pcols] = (mine[0, b, r] + got[1, b, r].astype(F32)).astype(BF16)
        whole_part(2 - inner, 0).wait_send()
    else:
        ahead = sorted(range(1, tp), key=lambda j: -min(j, tp - j))
        for j in ahead:
            t = (mt + j) % tp
            for b in range(blocks):
                parts[j, b] = project(t, b).astype(BF16)
                for i in (2 * b, 2 * b + 1):
                    send_part(j, i, got, mt, g_recv.at[mt], t).start()
        for b in range(blocks):
            mine[0, b] = project(mt, b)
        drain()
        for j in reversed(ahead):
            source = (mt + j) % tp
            whole_part(j, source).wait_recv()
            for b in range(blocks):
                mine[0, b] = mine[0, b] + got[source, b].astype(F32)
        for b in range(blocks):
            out_ref[:, b * pcols:(b + 1) * pcols] = mine[0, b].astype(BF16)
        for j in ahead:
            whole_part(j, 0).wait_send()


def solution(mesh):
    n, tp = mesh.shape["seq"], mesh.shape["tp"]

    def per_device(queries, keyvalues, stretch_order, block_table, proj_weight):
        rows, q_width = queries.shape
        kv_heads = keyvalues.shape[2] // HEAD
        width = proj_weight.shape[1] // tp
        pcols = 2 * HEAD if width % (2 * HEAD) == 0 else HEAD
        blocks = width // pcols
        group_rows = q_width // HEAD // kv_heads * rows
        line = tp == 4
        n_parts, n_got, n_mine = (3, 2, 3) if line else (tp, tp, 1)
        dma = pltpu.SemaphoreType.DMA
        args = (queries, keyvalues, stretch_order, block_table, proj_weight)
        return pl.pallas_call(
            functools.partial(kernel, n, tp),
            out_shape=pltpu.VMEM((rows, width), BF16),
            in_specs=[pl.BlockSpec(memory_space=pltpu.HBM)] * 5,
            out_specs=pl.BlockSpec(memory_space=pltpu.VMEM),
            scratch_shapes=[
                pltpu.SMEM(stretch_order.shape, jnp.int32),
                pltpu.SMEM(block_table.shape, jnp.int32),
                pltpu.VMEM((rows, q_width), BF16),
                pltpu.VMEM((kv_heads, HEAD, group_rows), BF16),
                pltpu.VMEM((n, kv_heads, 2, rows, HEAD), BF16),
                pltpu.VMEM(proj_weight.shape, BF16),
                pltpu.VMEM((kv_heads, 1, group_rows), F32),
                pltpu.VMEM((kv_heads, HEAD, group_rows), F32),
                pltpu.VMEM((kv_heads, 8, group_rows), F32),
                pltpu.VMEM((rows, q_width), BF16),
                pltpu.VMEM((n_mine, blocks, rows, pcols), F32),
                pltpu.VMEM((n_parts, blocks, rows, pcols), BF16),
                pltpu.VMEM((2, blocks, rows, pcols), BF16),
                pltpu.VMEM((n_got, blocks, rows, pcols), BF16),
                dma((5,)), dma((2,)), dma((max(n, 8 * kv_heads) if n == 8 else n,)), dma((1 + kv_heads,)),
                dma((n_parts,)), dma((2, 2 * blocks)), dma((n_got,)), dma((2 * blocks,)),
            ],
            compiler_params=pltpu.CompilerParams(
                collective_id=0, has_side_effects=True, vmem_limit_bytes=48 << 20,
            ),
        )(*(pltpu.with_memory_space_constraint(a, pltpu.HBM) for a in args))

    return jax.shard_map(
        per_device, mesh=mesh,
        in_specs=(P("seq", "tp"), P(None, "seq", "tp"), P(), P(), P("tp", None)),
        out_specs=P("seq", "tp"), check_vma=False,
    )
```

```python
import functools

import jax
import jax.numpy as jnp
from jax import lax
from jax.experimental import pallas as pl
from jax.experimental.pallas import tpu as pltpu
from jax.sharding import PartitionSpec as P

HEAD = 128
MASKED = -1e30
LOG2E = 1.4426950408889634
MESH = pl.DeviceIdType.MESH
F32 = jnp.float32
BF16 = jnp.bfloat16


def kernel(
    n, tp, q_hbm, kv_hbm, order_hbm, table_hbm, w_hbm, out_ref,
    order, table, q_in, q_t, kv_buf, w_buf, top_ref, acc, den, att, mine, parts, relay, got,
    in_sem, kv_send, kv_recv, hop_recv, p_send, r_recv, g_recv, f_recv, go,
):
    rows = q_in.shape[0]
    kv_heads = kv_buf.shape[1]
    q_heads = q_in.shape[1] // HEAD
    group = q_heads // kv_heads
    width = out_ref.shape[1]
    blocks, _, pcols = parts.shape[1:]
    half = rows // 2
    chips = n // 2
    me = lax.axis_index("seq")
    mt = lax.axis_index("tp")
    chip = me // 2
    core = me % 2
    partner = chip * 2 + 1 - core
    heads = range(kv_heads)

    own = [
        pltpu.make_async_copy(
            kv_hbm.at[i, :, slice(g * HEAD, (g + 1) * HEAD)], kv_buf.at[me, g, i], in_sem.at[4]
        )
        for g in heads for i in range(2)
    ]
    load_q = pltpu.make_async_copy(q_hbm, q_in, in_sem.at[0])
    load_w = pltpu.make_async_copy(w_hbm, w_buf, in_sem.at[1])
    load_order = pltpu.make_async_copy(order_hbm, order, in_sem.at[2])
    load_table = pltpu.make_async_copy(table_hbm, table, in_sem.at[3])
    for c in own:
        c.start()
    load_q.start()
    load_order.start()
    load_table.start()
    load_w.start()

    barrier = pltpu.get_barrier_semaphore()

    def peer(j):
        return ((chip + j) % chips) * 2 + core

    def each(lo, hi, body):
        if hi - lo <= 8:
            for j in range(lo, hi):
                body(j)
        else:
            lax.fori_loop(lo, hi, lambda j, c: (body(j), c)[1], 0)

    def greet_seq(s):
        pl.semaphore_signal(barrier, inc=1, device_id={"seq": s}, device_id_type=MESH)

    def greet_tp(t):
        pl.semaphore_signal(barrier, inc=1, device_id={"tp": t}, device_id_type=MESH)

    square = chips == 4
    chip_x, chip_y = chip % 2, chip // 2
    x0 = (chip_y * 2 + 1 - chip_x) * 2
    y0 = ((1 - chip_y) * 2 + chip_x) * 2
    d0 = ((1 - chip_y) * 2 + 1 - chip_x) * 2
    x1, y1, d1 = x0 + 1, y0 + 1, d0 + 1
    line = tp == 4
    side = mt // 2
    inner = mt % 2 * (1 - side) + (1 - mt % 2) * side

    def mirror(d):
        return d * (1 - side) + (3 - d) * side

    def entered(t):
        pl.semaphore_signal(barrier, inc=1, device_id={"seq": chip * 2, "tp": t}, device_id_type=MESH)

    split = square and line
    if split:
        @pl.when(core == 0)
        def _():
            greet_seq(partner)

        greet_seq(x0 + core)
        greet_seq(y0 + core)
        entered(mirror(2))
        entered(mirror(1 - inner))

        @pl.when(inner == 1)
        def _():
            entered(mirror(3))

        def tell_partner():
            pl.semaphore_signal(go, inc=1, device_id={"seq": partner}, device_id_type=MESH)

        @pl.when(core == 1)
        def _():
            pl.semaphore_wait(barrier, 3)
            tell_partner()

        @pl.when(core == 0)
        def _():
            pl.semaphore_wait(go, 1)
    else:
        greet_seq(partner)
        if square:
            for s in (x0, x1, y0, y1):
                greet_seq(s)
            seq_peers = 5
        else:
            each(1, chips, lambda j: greet_seq(peer(j)))
            seq_peers = chips
        if line:
            greet_tp(mirror(2))
            greet_tp(mirror(1 - inner))

            @pl.when(inner == 1)
            def _():
                greet_tp(mirror(3))

            tp_peers = 2 + inner
        else:
            for j in range(1, tp):
                greet_tp((mt + j) % tp)
            tp_peers = tp - 1
        pl.semaphore_wait(barrier, seq_peers + tp_peers)

    pltpu.make_async_copy(kv_buf.at[me], kv_buf.at[me], in_sem.at[4]).wait()

    def copy(ref, recv_sem, target, turn=0):
        return pltpu.make_async_remote_copy(
            src_ref=ref, dst_ref=ref, send_sem=kv_send.at[turn], recv_sem=recv_sem,
            device_id={"seq": target}, device_id_type=MESH,
        )

    def slot(s, target):
        return copy(kv_buf.at[s], kv_recv.at[s], target)

    def near_sem(axis, c, g):
        return kv_recv.at[(axis * 2 + c) * kv_heads + g]

    def far_sem(c, g, i):
        return kv_recv.at[((2 + c) * kv_heads + g) * 2 + i]

    def several(slots, recv_sem, turn=0):
        return copy(kv_buf.at[pl.ds(0, slots)], recv_sem, partner, turn)

    if square:
        for g in heads:
            for i in range(2):
                copy(kv_buf.at[me, g, i], hop_recv.at[0], partner).start()

        def send_near(i, x, y):
            for g in heads:
                copy(kv_buf.at[me, g, i], near_sem(0, core, g), x).start()
                copy(kv_buf.at[me, g, 1 - i], near_sem(1, core, g), y).start()

        send_near(0, x1, y1)
    else:
        slot(me, partner).start()
        each(1, chips, lambda j: slot(me, peer(j)).start())

    load_q.wait()
    for g in heads:
        for j in range(group):
            h = g * group + j
            q_t[g, :, j * rows:(j + 1) * rows] = q_in[:, h * HEAD:(h + 1) * HEAD].T

    load_order.wait()
    load_table.wait()
    my_stretch = order[me]
    scale = LOG2E / HEAD**0.5

    def bias_of(s):
        key_stretch = order[s]
        seen = jnp.logical_and(key_stretch < my_stretch, table[my_stretch, key_stretch] == 1)
        return jnp.where(seen, 0.0, MASKED).astype(F32)

    def attend(g, slots, first=False):
        queries = q_t[g]
        scores, tops, biases = [], [], []
        for i, s in enumerate(slots):
            part = jnp.dot(kv_buf[s, g, 0], queries, preferred_element_type=F32)
            if first and i == 0:
                k_pos = lax.broadcasted_iota(jnp.int32, part.shape, 0)
                q_pos = lax.broadcasted_iota(jnp.int32, part.shape, 1) % rows
                part = jnp.where(k_pos <= q_pos, part, MASKED)
                bias = 0.0
            else:
                bias = bias_of(s)
            scores.append(part)
            biases.append(bias)
            tops.append(jnp.max(part, axis=0, keepdims=True) + bias)
        new_top = functools.reduce(jnp.maximum, tops)
        if not first:
            old_top = top_ref[g]
            new_top = jnp.maximum(new_top, old_top)
        weights = jnp.concatenate(
            [jnp.exp2((p - (new_top - b)) * scale).astype(BF16) for p, b in zip(scores, biases)], axis=0
        )
        values = jnp.concatenate([kv_buf[s, g, 1] for s in slots], axis=0).T
        tall = jnp.concatenate([values, jnp.ones((16, values.shape[1]), BF16)], axis=0)
        added = jnp.dot(tall, weights, preferred_element_type=F32)
        if first:
            acc[g] = added[:HEAD]
            den[g] = added[HEAD:HEAD + 8]
        else:
            fade = jnp.exp2((old_top - new_top) * scale)
            acc[g] = acc[g] * fade + added[:HEAD]
            den[g] = den[g] * fade + added[HEAD:HEAD + 8]
        top_ref[g] = new_top

    if split:
        @pl.when(core == 0)
        def _():
            pl.semaphore_wait(barrier, 2 + 2 * (2 + inner))
            tell_partner()

        @pl.when(core == 1)
        def _():
            pl.semaphore_wait(go, 1)

    if square:
        send_near(1, x0, y0)
        several(1, hop_recv.at[0]).wait_recv()
    else:
        slot(partner, partner).wait_recv()
    for g in heads:
        attend(g, [me, partner], True)

    if square:
        near, far = [x1, y1, x0, y0], [d1, d0]

        def arrive(s, g, i, sem, onward=None, onward_sem=None):
            ref = kv_buf.at[s, g, i]
            copy(ref, sem, partner).wait_recv()
            if onward is not None:
                copy(ref, onward_sem, onward, 1).start()
            copy(ref, hop_recv.at[1 + g], partner, 1).start()

        @pl.when(core == 1)
        def _():
            for g in heads:
                for c, sx, sy in ((1, x1, y1), (0, x0, y0)):
                    arrive(sx, g, 0, near_sem(0, c, g), y0, far_sem(c, g, 0))
                    arrive(sy, g, 1, near_sem(1, c, g), x0, far_sem(c, g, 1))
            for g in heads:
                several(2, hop_recv.at[1 + g]).wait_recv()
                attend(g, near + far)

        @pl.when(core == 0)
        def _():
            for g in heads:
                for c, sx, sy in ((1, x1, y1), (0, x0, y0)):
                    arrive(sx, g, 1, near_sem(0, c, g))
                    arrive(sy, g, 0, near_sem(1, c, g))
                for c, s in ((1, d1), (0, d0)):
                    for i in range(2):
                        arrive(s, g, i, far_sem(c, g, i))
                several(1, hop_recv.at[1 + g]).wait_recv()
                attend(g, near + far)
    else:
        def step(j):
            s = ((chip - j + chips) % chips) * 2 + core
            other = ((chip - j + chips) % chips) * 2 + 1 - core
            slot(s, partner).wait_recv()
            slot(s, partner).start()
            slot(other, partner).wait_recv()
            for g in heads:
                attend(g, [s, other])

        each(1, chips, step)

    for g in heads:
        share = 1.0 / den[g][0:1]
        for j in range(group):
            h = g * group + j
            cols = slice(j * rows, (j + 1) * rows)
            att[:, h * HEAD:(h + 1) * HEAD] = (acc[g, :, cols] * share[:, cols]).astype(BF16).T

    load_w.wait()

    def project(t, b):
        cols = pl.ds(pl.multiple_of(t * width + b * pcols, pcols), pcols)
        return jnp.dot(att[...], w_buf[:, cols], preferred_element_type=F32)

    def part_of(ref, slot, i):
        return ref.at[slot, i // 2, pl.ds(i % 2 * half, half)]

    def send_part(c, i, dst, slot, recv_sem, target):
        return pltpu.make_async_remote_copy(
            src_ref=part_of(parts, c, i), dst_ref=part_of(dst, slot, i),
            send_sem=p_send.at[c], recv_sem=recv_sem,
            device_id={"tp": target}, device_id_type=MESH,
        )

    def whole_part(c, slot):
        return pltpu.make_async_remote_copy(
            src_ref=parts.at[c], dst_ref=got.at[slot], send_sem=p_send.at[c], recv_sem=g_recv.at[slot],
            device_id={"tp": mt}, device_id_type=MESH,
        )

    def drain():
        if square:
            several(3, hop_recv.at[0]).wait_send()
            several(4, hop_recv.at[0], 1).wait_send()
        else:
            several(n - 1, hop_recv.at[0]).wait_send()

    pieces = 2 * blocks
    if line:
        m0, m1, m2, m3 = (mirror(d) for d in range(4))

        def send_product(c, t, dst, slot, recv_sems, target):
            for b in range(blocks):
                parts[c, b] = project(t, b).astype(BF16)
                for i in (2 * b, 2 * b + 1):
                    send_part(c, i, dst, slot, recv_sems(i), target).start()

        def keep_own():
            for b in range(blocks):
                mine[0, b] = project(mt, b)

        @pl.when(inner == 0)
        def _():
            send_product(0, m3, relay, 0, lambda i: r_recv.at[0, i], m1)
            send_product(1, m2, relay, 1, lambda i: r_recv.at[1, i], m1)
            keep_own()

        @pl.when(jnp.logical_and(inner == 0, core == 0))
        def _():
            whole_part(1, 0).wait_send()

        @pl.when(inner == 0)
        def _():
            send_product(2, m1, got, 0, lambda i: g_recv.at[0], m1)

        @pl.when(inner == 1)
        def _():
            send_product(2, m0, got, 0, lambda i: g_recv.at[0], m0)
            for c, t in ((1, m3), (2, m2), (0, mt)):
                for b in range(blocks):
                    mine[c, b] = project(t, b)
            for c, target in ((0, m3), (1, m2)):
                for i in range(pieces):
                    b, r = i // 2, slice(i % 2 * half, (i % 2 + 1) * half)
                    send_part(2, i, relay, c, r_recv.at[c, i], m0).wait_recv()
                    parts[c, b, r] = (mine[1 + c, b, r] + relay[c, b, r].astype(F32)).astype(BF16)
                    send_part(c, i, got, 1, f_recv.at[i], target).start()

        drain()
        whole_part(0, 0).wait_send()
        whole_part(2, 0).wait_recv()
        for b in range(blocks):
            mine[0, b] = mine[0, b] + got[0, b].astype(F32)
        @pl.when(jnp.logical_or(inner == 1, core == 1))
        def _():
            whole_part(1 + inner, 0).wait_send()

        for i in range(pieces):
            b, r = i // 2, slice(i % 2 * half, (i % 2 + 1) * half)
            send_part(2, i, got, 1, f_recv.at[i], m0).wait_recv()
            out_ref[r, b * pcols:(b + 1) * pcols] = (mine[0, b, r] + got[1, b, r].astype(F32)).astype(BF16)
        whole_part(2 - inner, 0).wait_send()
    else:
        ahead = sorted(range(1, tp), key=lambda j: -min(j, tp - j))
        for j in ahead:
            t = (mt + j) % tp
            for b in range(blocks):
                parts[j, b] = project(t, b).astype(BF16)
                for i in (2 * b, 2 * b + 1):
                    send_part(j, i, got, mt, g_recv.at[mt], t).start()
        for b in range(blocks):
            mine[0, b] = project(mt, b)
        drain()
        for j in reversed(ahead):
            source = (mt + j) % tp
            whole_part(j, source).wait_recv()
            for b in range(blocks):
                mine[0, b] = mine[0, b] + got[source, b].astype(F32)
        for b in range(blocks):
            out_ref[:, b * pcols:(b + 1) * pcols] = mine[0, b].astype(BF16)
        for j in ahead:
            whole_part(j, 0).wait_send()


def solution(mesh):
    n, tp = mesh.shape["seq"], mesh.shape["tp"]

    def per_device(queries, keyvalues, stretch_order, block_table, proj_weight):
        rows, q_width = queries.shape
        kv_heads = keyvalues.shape[2] // HEAD
        width = proj_weight.shape[1] // tp
        pcols = 2 * HEAD if width % (2 * HEAD) == 0 else HEAD
        blocks = width // pcols
        group_rows = q_width // HEAD // kv_heads * rows
        line = tp == 4
        n_parts, n_got, n_mine = (3, 2, 3) if line else (tp, tp, 1)
        dma = pltpu.SemaphoreType.DMA
        args = (queries, keyvalues, stretch_order, block_table, proj_weight)
        return pl.pallas_call(
            functools.partial(kernel, n, tp),
            out_shape=pltpu.VMEM((rows, width), BF16),
            in_specs=[pl.BlockSpec(memory_space=pltpu.HBM)] * 5,
            out_specs=pl.BlockSpec(memory_space=pltpu.VMEM),
            scratch_shapes=[
                pltpu.SMEM(stretch_order.shape, jnp.int32),
                pltpu.SMEM(block_table.shape, jnp.int32),
                pltpu.VMEM((rows, q_width), BF16),
                pltpu.VMEM((kv_heads, HEAD, group_rows), BF16),
                pltpu.VMEM((n, kv_heads, 2, rows, HEAD), BF16),
                pltpu.VMEM(proj_weight.shape, BF16),
                pltpu.VMEM((kv_heads, 1, group_rows), F32),
                pltpu.VMEM((kv_heads, HEAD, group_rows), F32),
                pltpu.VMEM((kv_heads, 8, group_rows), F32),
                pltpu.VMEM((rows, q_width), BF16),
                pltpu.VMEM((n_mine, blocks, rows, pcols), F32),
                pltpu.VMEM((n_parts, blocks, rows, pcols), BF16),
                pltpu.VMEM((2, blocks, rows, pcols), BF16),
                pltpu.VMEM((n_got, blocks, rows, pcols), BF16),
                dma((5,)), dma((2,)), dma((max(n, 8 * kv_heads) if n == 8 else n,)), dma((1 + kv_heads,)),
                dma((n_parts,)), dma((2, 2 * blocks)), dma((n_got,)), dma((2 * blocks,)),
                pltpu.SemaphoreType.REGULAR,
            ],
            compiler_params=pltpu.CompilerParams(
                collective_id=0, has_side_effects=True, vmem_limit_bytes=48 << 20,
            ),
        )(*(pltpu.with_memory_space_constraint(a, pltpu.HBM) for a in args))

    return jax.shard_map(
        per_device, mesh=mesh,
        in_specs=(P("seq", "tp"), P(None, "seq", "tp"), P(), P(), P("tp", None)),
        out_specs=P("seq", "tp"), check_vma=False,
    )
```

```python
import functools

import jax
import jax.numpy as jnp
from jax import lax
from jax.experimental import pallas as pl
from jax.experimental.pallas import tpu as pltpu
from jax.sharding import PartitionSpec as P

HEAD = 128
MASKED = -1e30
LOG2E = 1.4426950408889634
MESH = pl.DeviceIdType.MESH
F32 = jnp.float32
BF16 = jnp.bfloat16


def kernel(
    n, tp, q_hbm, kv_hbm, order_hbm, table_hbm, w_hbm, out_ref,
    order, table, q_in, q_t, kv_buf, w_buf, top_ref, acc, den, att, mine, parts, relay, got,
    in_sem, kv_send, kv_recv, hop_recv, p_send, r_recv, g_recv, f_recv, go,
):
    rows = q_in.shape[0]
    kv_heads = kv_buf.shape[1]
    q_heads = q_in.shape[1] // HEAD
    group = q_heads // kv_heads
    width = out_ref.shape[1]
    blocks, _, pcols = parts.shape[1:]
    half = rows // 2
    chips = n // 2
    me = lax.axis_index("seq")
    mt = lax.axis_index("tp")
    chip = me // 2
    core = me % 2
    partner = chip * 2 + 1 - core
    heads = range(kv_heads)

    own = [
        pltpu.make_async_copy(
            kv_hbm.at[i, :, slice(g * HEAD, (g + 1) * HEAD)], kv_buf.at[me, g, i], in_sem.at[4]
        )
        for g in heads for i in range(2)
    ]
    load_q = pltpu.make_async_copy(q_hbm, q_in, in_sem.at[0])
    load_w = pltpu.make_async_copy(w_hbm, w_buf, in_sem.at[1])
    load_order = pltpu.make_async_copy(order_hbm, order, in_sem.at[2])
    load_table = pltpu.make_async_copy(table_hbm, table, in_sem.at[3])
    for c in own:
        c.start()
    load_q.start()
    load_order.start()
    load_table.start()
    load_w.start()

    barrier = pltpu.get_barrier_semaphore()

    def peer(j):
        return ((chip + j) % chips) * 2 + core

    def each(lo, hi, body):
        if hi - lo <= 8:
            for j in range(lo, hi):
                body(j)
        else:
            lax.fori_loop(lo, hi, lambda j, c: (body(j), c)[1], 0)

    def greet_seq(s):
        pl.semaphore_signal(barrier, inc=1, device_id={"seq": s}, device_id_type=MESH)

    def greet_tp(t):
        pl.semaphore_signal(barrier, inc=1, device_id={"tp": t}, device_id_type=MESH)

    square = chips == 4
    chip_x, chip_y = chip % 2, chip // 2
    x0 = (chip_y * 2 + 1 - chip_x) * 2
    y0 = ((1 - chip_y) * 2 + chip_x) * 2
    d0 = ((1 - chip_y) * 2 + 1 - chip_x) * 2
    x1, y1, d1 = x0 + 1, y0 + 1, d0 + 1
    line = tp == 4
    side = mt // 2
    inner = mt % 2 * (1 - side) + (1 - mt % 2) * side

    def mirror(d):
        return d * (1 - side) + (3 - d) * side

    def entered(t):
        pl.semaphore_signal(barrier, inc=1, device_id={"seq": chip * 2, "tp": t}, device_id_type=MESH)

    split = square and line
    if split:
        @pl.when(core == 0)
        def _():
            greet_seq(partner)

        greet_seq(x0 + core)
        greet_seq(y0 + core)
        entered(mirror(2))
        entered(mirror(1 - inner))

        @pl.when(inner == 1)
        def _():
            entered(mirror(3))

        def tell_partner():
            pl.semaphore_signal(go, inc=1, device_id={"seq": partner}, device_id_type=MESH)

        @pl.when(core == 1)
        def _():
            pl.semaphore_wait(barrier, 3)
            tell_partner()

        @pl.when(core == 0)
        def _():
            pl.semaphore_wait(go, 1)
    else:
        greet_seq(partner)
        if square:
            for s in (x0, x1, y0, y1):
                greet_seq(s)
            seq_peers = 5
        else:
            each(1, chips, lambda j: greet_seq(peer(j)))
            seq_peers = chips
        if line:
            greet_tp(mirror(2))
            greet_tp(mirror(1 - inner))

            @pl.when(inner == 1)
            def _():
                greet_tp(mirror(3))

            tp_peers = 2 + inner
        else:
            for j in range(1, tp):
                greet_tp((mt + j) % tp)
            tp_peers = tp - 1
        pl.semaphore_wait(barrier, seq_peers + tp_peers)

    pltpu.make_async_copy(kv_buf.at[me], kv_buf.at[me], in_sem.at[4]).wait()

    def copy(ref, recv_sem, target):
        return pltpu.make_async_remote_copy(
            src_ref=ref, dst_ref=ref, send_sem=kv_send, recv_sem=recv_sem,
            device_id={"seq": target}, device_id_type=MESH,
        )

    def slot(s, target):
        return copy(kv_buf.at[s], kv_recv.at[s], target)

    def relay_sem(axis, c, g):
        return kv_recv.at[(axis * 2 + c) * kv_heads + g]

    def near_sem(g):
        return kv_recv.at[g]

    def far_sem(g):
        return kv_recv.at[kv_heads + g]

    def several(slots, recv_sem):
        return copy(kv_buf.at[pl.ds(0, slots)], recv_sem, partner)

    if square:
        for g in heads:
            for i in range(2):
                copy(kv_buf.at[me, g, i], hop_recv.at[0], partner).start()

        for g in heads:
            copy(kv_buf.at[me, g, 0], relay_sem(0, core, g), x1).start()
            copy(kv_buf.at[me, g, 1], relay_sem(1, core, g), y1).start()
    else:
        slot(me, partner).start()
        each(1, chips, lambda j: slot(me, peer(j)).start())

    load_q.wait()
    for g in heads:
        for j in range(group):
            h = g * group + j
            q_t[g, :, j * rows:(j + 1) * rows] = q_in[:, h * HEAD:(h + 1) * HEAD].T

    load_order.wait()
    load_table.wait()
    my_stretch = order[me]
    scale = LOG2E / HEAD**0.5

    def bias_of(s):
        key_stretch = order[s]
        seen = jnp.logical_and(key_stretch < my_stretch, table[my_stretch, key_stretch] == 1)
        return jnp.where(seen, 0.0, MASKED).astype(F32)

    def attend(g, slots, first=False):
        queries = q_t[g]
        scores, tops, biases = [], [], []
        for i, s in enumerate(slots):
            part = jnp.dot(kv_buf[s, g, 0], queries, preferred_element_type=F32)
            if first and i == 0:
                k_pos = lax.broadcasted_iota(jnp.int32, part.shape, 0)
                q_pos = lax.broadcasted_iota(jnp.int32, part.shape, 1) % rows
                part = jnp.where(k_pos <= q_pos, part, MASKED)
                bias = 0.0
            else:
                bias = bias_of(s)
            scores.append(part)
            biases.append(bias)
            tops.append(jnp.max(part, axis=0, keepdims=True) + bias)
        new_top = functools.reduce(jnp.maximum, tops)
        if not first:
            old_top = top_ref[g]
            new_top = jnp.maximum(new_top, old_top)
        weights = jnp.concatenate(
            [jnp.exp2((p - (new_top - b)) * scale).astype(BF16) for p, b in zip(scores, biases)], axis=0
        )
        values = jnp.concatenate([kv_buf[s, g, 1] for s in slots], axis=0).T
        tall = jnp.concatenate([values, jnp.ones((16, values.shape[1]), BF16)], axis=0)
        added = jnp.dot(tall, weights, preferred_element_type=F32)
        if first:
            acc[g] = added[:HEAD]
            den[g] = added[HEAD:HEAD + 8]
        else:
            fade = jnp.exp2((old_top - new_top) * scale)
            acc[g] = acc[g] * fade + added[:HEAD]
            den[g] = den[g] * fade + added[HEAD:HEAD + 8]
        top_ref[g] = new_top

    if split:
        @pl.when(core == 0)
        def _():
            pl.semaphore_wait(barrier, 2 + 2 * (2 + inner))
            tell_partner()

        @pl.when(core == 1)
        def _():
            pl.semaphore_wait(go, 1)

    if square:
        for g in heads:
            copy(kv_buf.at[me, g, 1], near_sem(g), x0).start()
            copy(kv_buf.at[me, g, 0], near_sem(g), y0).start()
        several(1, hop_recv.at[0]).wait_recv()
    else:
        slot(partner, partner).wait_recv()
    for g in heads:
        attend(g, [me, partner], True)

    if square:
        near, far = [x1, y1, x0, y0], [d1, d0]

        def hand_over(s, g, i, hop):
            copy(kv_buf.at[s, g, i], hop_recv.at[hop], partner).start()

        @pl.when(core == 1)
        def _():
            for g in heads:
                for c, sx, sy in ((1, x1, y1), (0, x0, y0)):
                    for axis, s, target in ((0, sx, y0), (1, sy, x0)):
                        ref = kv_buf.at[s, g, axis]
                        copy(ref, relay_sem(axis, c, g), partner).wait_recv()
                        copy(ref, far_sem(g), target).start()
                        hand_over(s, g, axis, 1 + g)
            for slots, hop in ((near, 1), (far, 1 + kv_heads)):
                for g in heads:
                    several(1, hop_recv.at[hop + g]).wait_recv()
                    attend(g, slots)

        @pl.when(core == 0)
        def _():
            for g in heads:
                several(1, near_sem(g)).wait_recv()
                for sx, sy in ((x1, y1), (x0, y0)):
                    hand_over(sx, g, 1, 1 + g)
                    hand_over(sy, g, 0, 1 + g)
                several(1, hop_recv.at[1 + g]).wait_recv()
                attend(g, near)
            for g in heads:
                several(1, far_sem(g)).wait_recv()
                for s in far:
                    for i in range(2):
                        hand_over(s, g, i, 1 + kv_heads + g)
                attend(g, far)
    else:
        def step(j):
            s = ((chip - j + chips) % chips) * 2 + core
            other = ((chip - j + chips) % chips) * 2 + 1 - core
            slot(s, partner).wait_recv()
            slot(s, partner).start()
            slot(other, partner).wait_recv()
            for g in heads:
                attend(g, [s, other])

        each(1, chips, step)

    for g in heads:
        share = 1.0 / den[g][0:1]
        for j in range(group):
            h = g * group + j
            cols = slice(j * rows, (j + 1) * rows)
            att[:, h * HEAD:(h + 1) * HEAD] = (acc[g, :, cols] * share[:, cols]).astype(BF16).T

    load_w.wait()

    def project(t, b):
        cols = pl.ds(pl.multiple_of(t * width + b * pcols, pcols), pcols)
        return jnp.dot(att[...], w_buf[:, cols], preferred_element_type=F32)

    cuts = [(b, r * half, half) for b in range(blocks) for r in range(2)]
    b, r, count = cuts.pop()
    cuts += [(b, r, count // 2), (b, r + count // 2, count // 2)]

    def part_of(ref, slot, i):
        b, r, count = cuts[i]
        return ref.at[slot, b, pl.ds(r, count)]

    def send_part(c, i, dst, slot, recv_sem, target):
        return pltpu.make_async_remote_copy(
            src_ref=part_of(parts, c, i), dst_ref=part_of(dst, slot, i),
            send_sem=p_send.at[c], recv_sem=recv_sem,
            device_id={"tp": target}, device_id_type=MESH,
        )

    def whole_part(c, slot):
        return pltpu.make_async_remote_copy(
            src_ref=parts.at[c], dst_ref=got.at[slot], send_sem=p_send.at[c], recv_sem=g_recv.at[slot],
            device_id={"tp": mt}, device_id_type=MESH,
        )

    def drain():
        if square:
            several(7, hop_recv.at[0]).wait_send()
        else:
            several(n - 1, hop_recv.at[0]).wait_send()

    pieces = len(cuts)
    if line:
        m0, m1, m2, m3 = (mirror(d) for d in range(4))

        def send_product(c, t, dst, slot, recv_sems, target):
            for b in range(blocks):
                parts[c, b] = project(t, b).astype(BF16)
                for i in range(pieces):
                    if cuts[i][0] == b:
                        send_part(c, i, dst, slot, recv_sems(i), target).start()

        def keep_own():
            for b in range(blocks):
                mine[0, b] = project(mt, b)

        @pl.when(inner == 0)
        def _():
            send_product(0, m3, relay, 0, lambda i: r_recv.at[0, i], m1)
            send_product(1, m2, relay, 1, lambda i: r_recv.at[1, i], m1)
            keep_own()

        @pl.when(jnp.logical_and(inner == 0, core == 0))
        def _():
            whole_part(1, 0).wait_send()

        @pl.when(inner == 0)
        def _():
            send_product(2, m1, got, 0, lambda i: g_recv.at[0], m1)

        @pl.when(inner == 1)
        def _():
            send_product(2, m0, got, 0, lambda i: g_recv.at[0], m0)
            for c, t in ((1, m3), (2, m2), (0, mt)):
                for b in range(blocks):
                    mine[c, b] = project(t, b)
            for c, target in ((0, m3), (1, m2)):
                for i in range(pieces):
                    b, r = cuts[i][0], pl.ds(*cuts[i][1:])
                    send_part(2, i, relay, c, r_recv.at[c, i], m0).wait_recv()
                    parts[c, b, r] = (mine[1 + c, b, r] + relay[c, b, r].astype(F32)).astype(BF16)
                    send_part(c, i, got, 1, f_recv.at[i], target).start()

        drain()
        whole_part(0, 0).wait_send()
        whole_part(2, 0).wait_recv()
        for b in range(blocks):
            mine[0, b] = mine[0, b] + got[0, b].astype(F32)
        @pl.when(jnp.logical_or(inner == 1, core == 1))
        def _():
            whole_part(1 + inner, 0).wait_send()

        for i in range(pieces):
            b, r = cuts[i][0], pl.ds(*cuts[i][1:])
            send_part(2, i, got, 1, f_recv.at[i], m0).wait_recv()
            out_ref[r, b * pcols:(b + 1) * pcols] = (mine[0, b, r] + got[1, b, r].astype(F32)).astype(BF16)
        whole_part(2 - inner, 0).wait_send()
    else:
        ahead = sorted(range(1, tp), key=lambda j: -min(j, tp - j))
        for j in ahead:
            t = (mt + j) % tp
            for b in range(blocks):
                parts[j, b] = project(t, b).astype(BF16)
                for i in range(pieces):
                    if cuts[i][0] == b:
                        send_part(j, i, got, mt, g_recv.at[mt], t).start()
        for b in range(blocks):
            mine[0, b] = project(mt, b)
        drain()
        for j in reversed(ahead):
            source = (mt + j) % tp
            whole_part(j, source).wait_recv()
            for b in range(blocks):
                mine[0, b] = mine[0, b] + got[source, b].astype(F32)
        for b in range(blocks):
            out_ref[:, b * pcols:(b + 1) * pcols] = mine[0, b].astype(BF16)
        for j in ahead:
            whole_part(j, 0).wait_send()


def solution(mesh):
    n, tp = mesh.shape["seq"], mesh.shape["tp"]

    def per_device(queries, keyvalues, stretch_order, block_table, proj_weight):
        rows, q_width = queries.shape
        kv_heads = keyvalues.shape[2] // HEAD
        width = proj_weight.shape[1] // tp
        pcols = 2 * HEAD if width % (2 * HEAD) == 0 else HEAD
        blocks = width // pcols
        group_rows = q_width // HEAD // kv_heads * rows
        line = tp == 4
        n_parts, n_got, n_mine = (3, 2, 3) if line else (tp, tp, 1)
        dma = pltpu.SemaphoreType.DMA
        args = (queries, keyvalues, stretch_order, block_table, proj_weight)
        return pl.pallas_call(
            functools.partial(kernel, n, tp),
            out_shape=pltpu.VMEM((rows, width), BF16),
            in_specs=[pl.BlockSpec(memory_space=pltpu.HBM)] * 5,
            out_specs=pl.BlockSpec(memory_space=pltpu.VMEM),
            scratch_shapes=[
                pltpu.SMEM(stretch_order.shape, jnp.int32),
                pltpu.SMEM(block_table.shape, jnp.int32),
                pltpu.VMEM((rows, q_width), BF16),
                pltpu.VMEM((kv_heads, HEAD, group_rows), BF16),
                pltpu.VMEM((n, kv_heads, 2, rows, HEAD), BF16),
                pltpu.VMEM(proj_weight.shape, BF16),
                pltpu.VMEM((kv_heads, 1, group_rows), F32),
                pltpu.VMEM((kv_heads, HEAD, group_rows), F32),
                pltpu.VMEM((kv_heads, 8, group_rows), F32),
                pltpu.VMEM((rows, q_width), BF16),
                pltpu.VMEM((n_mine, blocks, rows, pcols), F32),
                pltpu.VMEM((n_parts, blocks, rows, pcols), BF16),
                pltpu.VMEM((2, blocks, rows, pcols), BF16),
                pltpu.VMEM((n_got, blocks, rows, pcols), BF16),
                dma((5,)), dma(()), dma((4 * kv_heads if n == 8 else n,)), dma((1 + 2 * kv_heads,)),
                dma((n_parts,)), dma((2, 2 * blocks + 1)), dma((1 if line else tp,)), dma((2 * blocks + 1,)),
                pltpu.SemaphoreType.REGULAR,
            ],
            compiler_params=pltpu.CompilerParams(
                collective_id=0, has_side_effects=True, vmem_limit_bytes=48 << 20,
            ),
        )(*(pltpu.with_memory_space_constraint(a, pltpu.HBM) for a in args))

    return jax.shard_map(
        per_device, mesh=mesh,
        in_specs=(P("seq", "tp"), P(None, "seq", "tp"), P(), P(), P("tp", None)),
        out_specs=P("seq", "tp"), check_vma=False,
    )
```

```python
import functools

import jax
import jax.numpy as jnp
from jax import lax
from jax.experimental import pallas as pl
from jax.experimental.pallas import tpu as pltpu
from jax.sharding import PartitionSpec as P

HEAD = 128
MASKED = -1e30
LOG2E = 1.4426950408889634
MESH = pl.DeviceIdType.MESH
F32 = jnp.float32
BF16 = jnp.bfloat16


def kernel(
    n, tp, q_hbm, kv_hbm, order_hbm, table_hbm, w_hbm, out_ref,
    order, table, q_in, q_t, kv_buf, w_buf, top_ref, acc, den, att, mine, parts, relay, got,
    in_sem, kv_send, kv_recv, hop_recv, p_send, r_recv, g_recv, f_recv, go,
):
    rows = q_in.shape[0]
    kv_heads = kv_buf.shape[1]
    q_heads = q_in.shape[1] // HEAD
    group = q_heads // kv_heads
    width = out_ref.shape[1]
    blocks, _, pcols = parts.shape[1:]
    half = rows // 2
    chips = n // 2
    me = lax.axis_index("seq")
    mt = lax.axis_index("tp")
    chip = me // 2
    core = me % 2
    partner = chip * 2 + 1 - core
    heads = range(kv_heads)

    own = [
        pltpu.make_async_copy(
            kv_hbm.at[i, :, slice(g * HEAD, (g + 1) * HEAD)], kv_buf.at[me, g, i], in_sem.at[4]
        )
        for g in heads for i in range(2)
    ]
    load_q = pltpu.make_async_copy(q_hbm, q_in, in_sem.at[0])
    load_w = pltpu.make_async_copy(w_hbm, w_buf, in_sem.at[1])
    load_order = pltpu.make_async_copy(order_hbm, order, in_sem.at[2])
    load_table = pltpu.make_async_copy(table_hbm, table, in_sem.at[3])
    for c in own:
        c.start()
    load_q.start()
    load_order.start()
    load_table.start()
    load_w.start()

    barrier = pltpu.get_barrier_semaphore()

    def peer(j):
        return ((chip + j) % chips) * 2 + core

    def each(lo, hi, body):
        if hi - lo <= 8:
            for j in range(lo, hi):
                body(j)
        else:
            lax.fori_loop(lo, hi, lambda j, c: (body(j), c)[1], 0)

    def greet_seq(s):
        pl.semaphore_signal(barrier, inc=1, device_id={"seq": s}, device_id_type=MESH)

    def greet_tp(t):
        pl.semaphore_signal(barrier, inc=1, device_id={"tp": t}, device_id_type=MESH)

    square = chips == 4
    chip_x, chip_y = chip % 2, chip // 2
    x0 = (chip_y * 2 + 1 - chip_x) * 2
    y0 = ((1 - chip_y) * 2 + chip_x) * 2
    d0 = ((1 - chip_y) * 2 + 1 - chip_x) * 2
    x1, y1, d1 = x0 + 1, y0 + 1, d0 + 1
    line = tp == 4
    side = mt // 2
    inner = mt % 2 * (1 - side) + (1 - mt % 2) * side

    def mirror(d):
        return d * (1 - side) + (3 - d) * side

    def entered(t):
        pl.semaphore_signal(barrier, inc=1, device_id={"seq": chip * 2, "tp": t}, device_id_type=MESH)

    split = square and line
    if split:
        @pl.when(core == 0)
        def _():
            greet_seq(partner)

        greet_seq(x0 + core)
        greet_seq(y0 + core)
        entered(mirror(2))
        entered(mirror(1 - inner))

        @pl.when(inner == 1)
        def _():
            entered(mirror(3))

        def tell_partner():
            pl.semaphore_signal(go, inc=1, device_id={"seq": partner}, device_id_type=MESH)

        @pl.when(core == 1)
        def _():
            pl.semaphore_wait(barrier, 3)
            tell_partner()

        @pl.when(core == 0)
        def _():
            pl.semaphore_wait(go, 1)
    else:
        greet_seq(partner)
        if square:
            for s in (x0, x1, y0, y1):
                greet_seq(s)
            seq_peers = 5
        else:
            each(1, chips, lambda j: greet_seq(peer(j)))
            seq_peers = chips
        if line:
            greet_tp(mirror(2))
            greet_tp(mirror(1 - inner))

            @pl.when(inner == 1)
            def _():
                greet_tp(mirror(3))

            tp_peers = 2 + inner
        else:
            for j in range(1, tp):
                greet_tp((mt + j) % tp)
            tp_peers = tp - 1
        pl.semaphore_wait(barrier, seq_peers + tp_peers)

    pltpu.make_async_copy(kv_buf.at[me], kv_buf.at[me], in_sem.at[4]).wait()

    def copy(ref, recv_sem, target):
        return pltpu.make_async_remote_copy(
            src_ref=ref, dst_ref=ref, send_sem=kv_send, recv_sem=recv_sem,
            device_id={"seq": target}, device_id_type=MESH,
        )

    def slot(s, target):
        return copy(kv_buf.at[s], kv_recv.at[s], target)

    def relay_sem(axis, c, g):
        return kv_recv.at[(axis * 2 + c) * kv_heads + g]

    def near_sem(g):
        return kv_recv.at[g]

    def far_sem(g):
        return kv_recv.at[kv_heads + g]

    def several(slots, recv_sem):
        return copy(kv_buf.at[pl.ds(0, slots)], recv_sem, partner)

    if square:

        for g in heads:
            copy(kv_buf.at[me, g, 0], relay_sem(0, core, g), x1).start()
            copy(kv_buf.at[me, g, 1], relay_sem(1, core, g), y1).start()
        for g in heads:
            for i in range(2):
                copy(kv_buf.at[me, g, i], hop_recv.at[0], partner).start()
    else:
        slot(me, partner).start()
        each(1, chips, lambda j: slot(me, peer(j)).start())

    load_q.wait()
    for g in heads:
        for j in range(group):
            h = g * group + j
            q_t[g, :, j * rows:(j + 1) * rows] = q_in[:, h * HEAD:(h + 1) * HEAD].T

    load_order.wait()
    load_table.wait()
    my_stretch = order[me]
    scale = LOG2E / HEAD**0.5

    def bias_of(s):
        key_stretch = order[s]
        seen = jnp.logical_and(key_stretch < my_stretch, table[my_stretch, key_stretch] == 1)
        return jnp.where(seen, 0.0, MASKED).astype(F32)

    def attend(g, slots, first=False):
        queries = q_t[g]
        scores, tops, biases = [], [], []
        for i, s in enumerate(slots):
            part = jnp.dot(kv_buf[s, g, 0], queries, preferred_element_type=F32)
            if first and i == 0:
                k_pos = lax.broadcasted_iota(jnp.int32, part.shape, 0)
                q_pos = lax.broadcasted_iota(jnp.int32, part.shape, 1) % rows
                part = jnp.where(k_pos <= q_pos, part, MASKED)
                bias = 0.0
            else:
                bias = bias_of(s)
            scores.append(part)
            biases.append(bias)
            tops.append(jnp.max(part, axis=0, keepdims=True) + bias)
        new_top = functools.reduce(jnp.maximum, tops)
        if not first:
            old_top = top_ref[g]
            new_top = jnp.maximum(new_top, old_top)
        weights = jnp.concatenate(
            [jnp.exp2((p - (new_top - b)) * scale).astype(BF16) for p, b in zip(scores, biases)], axis=0
        )
        values = jnp.concatenate([kv_buf[s, g, 1] for s in slots], axis=0).T
        tall = jnp.concatenate([values, jnp.ones((16, values.shape[1]), BF16)], axis=0)
        added = jnp.dot(tall, weights, preferred_element_type=F32)
        if first:
            acc[g] = added[:HEAD]
            den[g] = added[HEAD:HEAD + 8]
        else:
            fade = jnp.exp2((old_top - new_top) * scale)
            acc[g] = acc[g] * fade + added[:HEAD]
            den[g] = den[g] * fade + added[HEAD:HEAD + 8]
        top_ref[g] = new_top

    if split:
        @pl.when(core == 0)
        def _():
            pl.semaphore_wait(barrier, 2 + 2 * (2 + inner))
            tell_partner()

        @pl.when(core == 1)
        def _():
            pl.semaphore_wait(go, 1)

    def begin():
        for g in heads:
            attend(g, [me, partner], True)

    def normalise(g):
        share = 1.0 / den[g][0:1]
        for j in range(group):
            h = g * group + j
            cols = slice(j * rows, (j + 1) * rows)
            att[:, h * HEAD:(h + 1) * HEAD] = (acc[g, :, cols] * share[:, cols]).astype(BF16).T

    last = kv_heads - 1
    done = last * group * HEAD
    early = split and done > 0
    first_part = mirror(3) * (1 - inner) + mirror(0) * inner

    def columns(t):
        return pl.ds(pl.multiple_of(t * width, width), width)

    def look_ahead(g):
        if early and g == last:
            for k in range(last):
                normalise(k)
            ahead = jnp.dot(att[:, :done], w_buf[:done, columns(first_part)], preferred_element_type=F32)
            for b in range(blocks):
                mine[0, b] = ahead[:, b * pcols:(b + 1) * pcols]

    if square:
        for g in heads:
            copy(kv_buf.at[me, g, 1], near_sem(g), x0).start()
            copy(kv_buf.at[me, g, 0], near_sem(g), y0).start()
        near, far = [x1, y1, x0, y0], [d1, d0]

        def hand_over(s, g, i, hop):
            copy(kv_buf.at[s, g, i], hop_recv.at[hop], partner).start()

        @pl.when(core == 1)
        def _():
            for g in heads:
                for c, sx, sy in ((1, x1, y1), (0, x0, y0)):
                    for axis, s, target in ((0, sx, y0), (1, sy, x0)):
                        ref = kv_buf.at[s, g, axis]
                        copy(ref, relay_sem(axis, c, g), partner).wait_recv()
                        copy(ref, far_sem(g), target).start()
                        hand_over(s, g, axis, 1 + g)
            several(1, hop_recv.at[0]).wait_recv()
            begin()
            load_w.wait()
            for slots, hop in ((near, 1), (far, 1 + kv_heads)):
                for g in heads:
                    several(1, hop_recv.at[hop + g]).wait_recv()
                    if slots is far:
                        look_ahead(g)
                    attend(g, slots)

        @pl.when(core == 0)
        def _():
            several(1, hop_recv.at[0]).wait_recv()
            begin()
            load_w.wait()
            for g in heads:
                several(1, near_sem(g)).wait_recv()
                for sx, sy in ((x1, y1), (x0, y0)):
                    hand_over(sx, g, 1, 1 + g)
                    hand_over(sy, g, 0, 1 + g)
                several(1, hop_recv.at[1 + g]).wait_recv()
                attend(g, near)
            for g in heads:
                several(1, far_sem(g)).wait_recv()
                for s in far:
                    for i in range(2):
                        hand_over(s, g, i, 1 + kv_heads + g)
                look_ahead(g)
                attend(g, far)
    else:
        slot(partner, partner).wait_recv()
        begin()
        load_w.wait()

        def step(j):
            s = ((chip - j + chips) % chips) * 2 + core
            other = ((chip - j + chips) % chips) * 2 + 1 - core
            slot(s, partner).wait_recv()
            slot(s, partner).start()
            slot(other, partner).wait_recv()
            for g in heads:
                attend(g, [s, other])

        each(1, chips, step)

    for g in [last] if early else heads:
        normalise(g)

    def project(t, ref, slot, ready=0):
        product = jnp.dot(att[:, ready:], w_buf[ready:, columns(t)], preferred_element_type=F32)
        for b in range(blocks):
            block = product[:, b * pcols:(b + 1) * pcols]
            ref[slot, b] = (block + mine[0, b] if ready else block).astype(ref.dtype)

    cuts = [(b, r * half // 2, half // 2) for b in range(blocks) for r in range(4)]

    def part_of(ref, slot, i):
        b, r, count = cuts[i]
        return ref.at[slot, b, pl.ds(r, count)]

    def send_part(c, i, dst, slot, recv_sem, target):
        return pltpu.make_async_remote_copy(
            src_ref=part_of(parts, c, i), dst_ref=part_of(dst, slot, i),
            send_sem=p_send.at[c], recv_sem=recv_sem,
            device_id={"tp": target}, device_id_type=MESH,
        )

    def whole_part(c, slot):
        return pltpu.make_async_remote_copy(
            src_ref=parts.at[c], dst_ref=got.at[slot], send_sem=p_send.at[c], recv_sem=g_recv.at[slot],
            device_id={"tp": mt}, device_id_type=MESH,
        )

    def drain():
        if square:
            several(7, hop_recv.at[0]).wait_send()
        else:
            several(n - 1, hop_recv.at[0]).wait_send()

    pieces = len(cuts)
    if line:
        m0, m1, m2, m3 = (mirror(d) for d in range(4))

        def send_product(c, t, dst, slot, recv_sems, target, ready=0):
            project(t, parts, c, ready)
            for i in range(pieces):
                send_part(c, i, dst, slot, recv_sems(i), target).start()

        def keep_own():
            project(mt, mine, 0)

        @pl.when(inner == 0)
        def _():
            send_product(0, m3, relay, 0, lambda i: r_recv.at[0, i], m1, done if early else 0)
            send_product(1, m2, relay, 1, lambda i: r_recv.at[1, i], m1)
            keep_own()

        @pl.when(jnp.logical_and(inner == 0, core == 0))
        def _():
            whole_part(1, 0).wait_send()

        @pl.when(inner == 0)
        def _():
            send_product(2, m1, got, 0, lambda i: g_recv.at[0], m1)

        @pl.when(inner == 1)
        def _():
            send_product(2, m0, got, 0, lambda i: g_recv.at[0], m0, done if early else 0)
            for c, t in ((1, m3), (2, m2), (0, mt)):
                project(t, mine, c)
            for c, target in ((0, m3), (1, m2)):
                for i in range(pieces):
                    b, r = cuts[i][0], pl.ds(*cuts[i][1:])
                    send_part(2, i, relay, c, r_recv.at[c, i], m0).wait_recv()
                    parts[c, b, r] = (mine[1 + c, b, r] + relay[c, b, r].astype(F32)).astype(BF16)
                    send_part(c, i, got, 1, f_recv.at[i], target).start()

        drain()
        whole_part(0, 0).wait_send()
        whole_part(2, 0).wait_recv()
        for b in range(blocks):
            mine[0, b] = mine[0, b] + got[0, b].astype(F32)
        @pl.when(jnp.logical_or(inner == 1, core == 1))
        def _():
            whole_part(1 + inner, 0).wait_send()

        for i in range(pieces):
            b, r = cuts[i][0], pl.ds(*cuts[i][1:])
            send_part(2, i, got, 1, f_recv.at[i], m0).wait_recv()
            out_ref[r, b * pcols:(b + 1) * pcols] = (mine[0, b, r] + got[1, b, r].astype(F32)).astype(BF16)
        whole_part(2 - inner, 0).wait_send()
    else:
        ahead = sorted(range(1, tp), key=lambda j: -min(j, tp - j))
        for j in ahead:
            t = (mt + j) % tp
            project(t, parts, j)
            for i in range(pieces):
                send_part(j, i, got, mt, g_recv.at[mt], t).start()
        project(mt, mine, 0)
        drain()
        for j in reversed(ahead):
            source = (mt + j) % tp
            whole_part(j, source).wait_recv()
            for b in range(blocks):
                mine[0, b] = mine[0, b] + got[source, b].astype(F32)
        for b in range(blocks):
            out_ref[:, b * pcols:(b + 1) * pcols] = mine[0, b].astype(BF16)
        for j in ahead:
            whole_part(j, 0).wait_send()


def solution(mesh):
    n, tp = mesh.shape["seq"], mesh.shape["tp"]

    def per_device(queries, keyvalues, stretch_order, block_table, proj_weight):
        rows, q_width = queries.shape
        kv_heads = keyvalues.shape[2] // HEAD
        width = proj_weight.shape[1] // tp
        pcols = 2 * HEAD if width % (2 * HEAD) == 0 else HEAD
        blocks = width // pcols
        group_rows = q_width // HEAD // kv_heads * rows
        line = tp == 4
        n_parts, n_got, n_mine = (3, 2, 3) if line else (tp, tp, 1)
        dma = pltpu.SemaphoreType.DMA
        args = (queries, keyvalues, stretch_order, block_table, proj_weight)
        return pl.pallas_call(
            functools.partial(kernel, n, tp),
            out_shape=pltpu.VMEM((rows, width), BF16),
            in_specs=[pl.BlockSpec(memory_space=pltpu.HBM)] * 5,
            out_specs=pl.BlockSpec(memory_space=pltpu.VMEM),
            scratch_shapes=[
                pltpu.SMEM(stretch_order.shape, jnp.int32),
                pltpu.SMEM(block_table.shape, jnp.int32),
                pltpu.VMEM((rows, q_width), BF16),
                pltpu.VMEM((kv_heads, HEAD, group_rows), BF16),
                pltpu.VMEM((n, kv_heads, 2, rows, HEAD), BF16),
                pltpu.VMEM(proj_weight.shape, BF16),
                pltpu.VMEM((kv_heads, 1, group_rows), F32),
                pltpu.VMEM((kv_heads, HEAD, group_rows), F32),
                pltpu.VMEM((kv_heads, 8, group_rows), F32),
                pltpu.VMEM((rows, q_width), BF16),
                pltpu.VMEM((n_mine, blocks, rows, pcols), F32),
                pltpu.VMEM((n_parts, blocks, rows, pcols), BF16),
                pltpu.VMEM((2, blocks, rows, pcols), BF16),
                pltpu.VMEM((n_got, blocks, rows, pcols), BF16),
                dma((5,)), dma(()), dma((4 * kv_heads if n == 8 else n,)), dma((1 + 2 * kv_heads,)),
                dma((n_parts,)), dma((2, 4 * blocks)), dma((1 if line else tp,)), dma((4 * blocks,)),
                pltpu.SemaphoreType.REGULAR,
            ],
            compiler_params=pltpu.CompilerParams(
                collective_id=0, has_side_effects=True, vmem_limit_bytes=48 << 20,
            ),
        )(*(pltpu.with_memory_space_constraint(a, pltpu.HBM) for a in args))

    return jax.shard_map(
        per_device, mesh=mesh,
        in_specs=(P("seq", "tp"), P(None, "seq", "tp"), P(), P(), P("tp", None)),
        out_specs=P("seq", "tp"), check_vma=False,
    )
```

```python
import functools

import jax
import jax.numpy as jnp
from jax import lax
from jax.experimental import pallas as pl
from jax.experimental.pallas import tpu as pltpu
from jax.sharding import PartitionSpec as P

HEAD = 128
MASKED = -1e30
LOG2E = 1.4426950408889634
MESH = pl.DeviceIdType.MESH
F32 = jnp.float32
BF16 = jnp.bfloat16


def kernel(
    n, tp, q_hbm, kv_hbm, order_hbm, table_hbm, w_hbm, out_ref,
    order, table, q_in, q_t, kv_buf, w_buf, top_ref, acc, den, att, mine, parts, relay, got,
    in_sem, kv_send, kv_recv, hop_recv, p_send, r_recv, g_recv, f_recv, go,
):
    rows = q_in.shape[0]
    kv_heads = kv_buf.shape[1]
    q_heads = q_in.shape[1] // HEAD
    group = q_heads // kv_heads
    width = out_ref.shape[1]
    blocks, _, pcols = parts.shape[1:]
    half = rows // 2
    chips = n // 2
    me = lax.axis_index("seq")
    mt = lax.axis_index("tp")
    chip = me // 2
    core = me % 2
    partner = chip * 2 + 1 - core
    heads = range(kv_heads)

    own = [
        pltpu.make_async_copy(
            kv_hbm.at[i, :, slice(g * HEAD, (g + 1) * HEAD)], kv_buf.at[me, g, i], in_sem.at[4]
        )
        for g in heads for i in range(2)
    ]
    load_q = pltpu.make_async_copy(q_hbm, q_in, in_sem.at[0])
    load_w = pltpu.make_async_copy(w_hbm, w_buf, in_sem.at[1])
    load_order = pltpu.make_async_copy(order_hbm, order, in_sem.at[2])
    load_table = pltpu.make_async_copy(table_hbm, table, in_sem.at[3])
    for c in own:
        c.start()
    load_q.start()
    load_order.start()
    load_table.start()
    load_w.start()

    barrier = pltpu.get_barrier_semaphore()

    def peer(j):
        return ((chip + j) % chips) * 2 + core

    def each(lo, hi, body):
        if hi - lo <= 8:
            for j in range(lo, hi):
                body(j)
        else:
            lax.fori_loop(lo, hi, lambda j, c: (body(j), c)[1], 0)

    def greet_seq(s):
        pl.semaphore_signal(barrier, inc=1, device_id={"seq": s}, device_id_type=MESH)

    def greet_tp(t):
        pl.semaphore_signal(barrier, inc=1, device_id={"tp": t}, device_id_type=MESH)

    square = chips == 4
    chip_x, chip_y = chip % 2, chip // 2
    x0 = (chip_y * 2 + 1 - chip_x) * 2
    y0 = ((1 - chip_y) * 2 + chip_x) * 2
    d0 = ((1 - chip_y) * 2 + 1 - chip_x) * 2
    x1, y1, d1 = x0 + 1, y0 + 1, d0 + 1
    line = tp == 4
    side = mt // 2
    inner = mt % 2 * (1 - side) + (1 - mt % 2) * side

    def mirror(d):
        return d * (1 - side) + (3 - d) * side

    def entered(t):
        pl.semaphore_signal(barrier, inc=1, device_id={"seq": chip * 2, "tp": t}, device_id_type=MESH)

    split = square and line
    if split:
        @pl.when(core == 0)
        def _():
            greet_seq(partner)

        greet_seq(x0 + core)
        greet_seq(y0 + core)
        entered(mirror(2))
        entered(mirror(1 - inner))

        @pl.when(inner == 1)
        def _():
            entered(mirror(3))

        def tell_partner():
            pl.semaphore_signal(go, inc=1, device_id={"seq": partner}, device_id_type=MESH)

        @pl.when(core == 1)
        def _():
            pl.semaphore_wait(barrier, 3)
            tell_partner()

        @pl.when(core == 0)
        def _():
            pl.semaphore_wait(go, 1)
    else:
        greet_seq(partner)
        if square:
            for s in (x0, x1, y0, y1):
                greet_seq(s)
            seq_peers = 5
        else:
            each(1, chips, lambda j: greet_seq(peer(j)))
            seq_peers = chips
        if line:
            greet_tp(mirror(2))
            greet_tp(mirror(1 - inner))

            @pl.when(inner == 1)
            def _():
                greet_tp(mirror(3))

            tp_peers = 2 + inner
        else:
            for j in range(1, tp):
                greet_tp((mt + j) % tp)
            tp_peers = tp - 1
        pl.semaphore_wait(barrier, seq_peers + tp_peers)

    pltpu.make_async_copy(kv_buf.at[me], kv_buf.at[me], in_sem.at[4]).wait()

    def copy(ref, recv_sem, target):
        return pltpu.make_async_remote_copy(
            src_ref=ref, dst_ref=ref, send_sem=kv_send, recv_sem=recv_sem,
            device_id={"seq": target}, device_id_type=MESH,
        )

    def slot(s, target):
        return copy(kv_buf.at[s], kv_recv.at[s], target)

    def relay_sem(axis, c, g):
        return kv_recv.at[(axis * 2 + c) * kv_heads + g]

    def near_sem(c, g):
        return kv_recv.at[c * kv_heads + g]

    def far_sem(c, g):
        return kv_recv.at[(2 + c) * kv_heads + g]

    def pair(recv_sem):
        return copy(kv_buf.at[0, 0], recv_sem, partner)

    def several(slots, recv_sem):
        return copy(kv_buf.at[pl.ds(0, slots)], recv_sem, partner)

    if square:

        for g in heads:
            copy(kv_buf.at[me, g, 0], relay_sem(0, core, g), x1).start()
            copy(kv_buf.at[me, g, 1], relay_sem(1, core, g), y1).start()
        for g in heads:
            for i in range(2):
                copy(kv_buf.at[me, g, i], hop_recv.at[0], partner).start()
    else:
        slot(me, partner).start()
        each(1, chips, lambda j: slot(me, peer(j)).start())

    load_q.wait()
    for g in heads:
        for j in range(group):
            h = g * group + j
            q_t[g, :, j * rows:(j + 1) * rows] = q_in[:, h * HEAD:(h + 1) * HEAD].T

    load_order.wait()
    load_table.wait()
    my_stretch = order[me]
    scale = LOG2E / HEAD**0.5

    def bias_of(s):
        key_stretch = order[s]
        seen = jnp.logical_and(key_stretch < my_stretch, table[my_stretch, key_stretch] == 1)
        return jnp.where(seen, 0.0, MASKED).astype(F32)

    def attend(g, slots, first=False):
        queries = q_t[g]
        scores, tops, biases = [], [], []
        for i, s in enumerate(slots):
            part = jnp.dot(kv_buf[s, g, 0], queries, preferred_element_type=F32)
            if first and i == 0:
                k_pos = lax.broadcasted_iota(jnp.int32, part.shape, 0)
                q_pos = lax.broadcasted_iota(jnp.int32, part.shape, 1) % rows
                part = jnp.where(k_pos <= q_pos, part, MASKED)
                bias = 0.0
            else:
                bias = bias_of(s)
            scores.append(part)
            biases.append(bias)
            tops.append(jnp.max(part, axis=0, keepdims=True) + bias)
        new_top = functools.reduce(jnp.maximum, tops)
        if not first:
            old_top = top_ref[g]
            new_top = jnp.maximum(new_top, old_top)
        weights = jnp.concatenate(
            [jnp.exp2((p - (new_top - b)) * scale).astype(BF16) for p, b in zip(scores, biases)], axis=0
        )
        values = jnp.concatenate([kv_buf[s, g, 1] for s in slots], axis=0).T
        tall = jnp.concatenate([values, jnp.ones((16, values.shape[1]), BF16)], axis=0)
        added = jnp.dot(tall, weights, preferred_element_type=F32)
        if first:
            acc[g] = added[:HEAD]
            den[g] = added[HEAD:HEAD + 8]
        else:
            fade = jnp.exp2((old_top - new_top) * scale)
            acc[g] = acc[g] * fade + added[:HEAD]
            den[g] = den[g] * fade + added[HEAD:HEAD + 8]
        top_ref[g] = new_top

    if split:
        @pl.when(core == 0)
        def _():
            pl.semaphore_wait(barrier, 2 + 2 * (2 + inner))
            tell_partner()

        @pl.when(core == 1)
        def _():
            pl.semaphore_wait(go, 1)

    def begin():
        for g in heads:
            attend(g, [me, partner], True)

    def normalise(g):
        share = 1.0 / den[g][0:1]
        for j in range(group):
            h = g * group + j
            cols = slice(j * rows, (j + 1) * rows)
            att[:, h * HEAD:(h + 1) * HEAD] = (acc[g, :, cols] * share[:, cols]).astype(BF16).T

    last = kv_heads - 1
    done = last * group * HEAD
    early = split and done > 0
    first_part = mirror(3) * (1 - inner) + mirror(0) * inner

    def columns(t):
        return pl.ds(pl.multiple_of(t * width, width), width)

    def look_ahead(g):
        if early and g == last:
            for k in range(last):
                normalise(k)
            ahead = jnp.dot(att[:, :done], w_buf[:done, columns(first_part)], preferred_element_type=F32)
            for b in range(blocks):
                mine[0, b] = ahead[:, b * pcols:(b + 1) * pcols]

    if square:
        for g in heads:
            copy(kv_buf.at[me, g, 1], near_sem(core, g), x0).start()
            copy(kv_buf.at[me, g, 0], near_sem(core, g), y0).start()
        near, far = [x1, y1, x0, y0], [d1, d0]

        def hand_over(s, g, i, hop):
            copy(kv_buf.at[s, g, i], hop_recv.at[hop], partner).start()

        @pl.when(core == 1)
        def _():
            for g in heads:
                for c, sx, sy in ((1, x1, y1), (0, x0, y0)):
                    for axis, s, target in ((0, sx, y0), (1, sy, x0)):
                        ref = kv_buf.at[s, g, axis]
                        copy(ref, relay_sem(axis, c, g), partner).wait_recv()
                        copy(ref, far_sem(c, g), target).start()
                        hand_over(s, g, axis, 1 + g)
            several(1, hop_recv.at[0]).wait_recv()
            begin()
            load_w.wait()
            for slots, hop in ((near, 1), (far, 1 + kv_heads)):
                for g in heads:
                    several(1, hop_recv.at[hop + g]).wait_recv()
                    if slots is far:
                        look_ahead(g)
                    attend(g, slots)

        @pl.when(core == 0)
        def _():
            several(1, hop_recv.at[0]).wait_recv()
            begin()
            load_w.wait()
            for g in heads:
                for c, sx, sy in ((1, x1, y1), (0, x0, y0)):
                    pair(near_sem(c, g)).wait_recv()
                    hand_over(sx, g, 1, 1 + g)
                    hand_over(sy, g, 0, 1 + g)
                several(1, hop_recv.at[1 + g]).wait_recv()
                attend(g, near)
            for g in heads:
                for c, s in ((1, d1), (0, d0)):
                    pair(far_sem(c, g)).wait_recv()
                    for i in range(2):
                        hand_over(s, g, i, 1 + kv_heads + g)
                look_ahead(g)
                attend(g, far)
    else:
        slot(partner, partner).wait_recv()
        begin()
        load_w.wait()

        def step(j):
            s = ((chip - j + chips) % chips) * 2 + core
            other = ((chip - j + chips) % chips) * 2 + 1 - core
            slot(s, partner).wait_recv()
            slot(s, partner).start()
            slot(other, partner).wait_recv()
            for g in heads:
                attend(g, [s, other])

        each(1, chips, step)

    for g in [last] if early else heads:
        normalise(g)

    def project(t, ref, slot, ready=0):
        product = jnp.dot(att[:, ready:], w_buf[ready:, columns(t)], preferred_element_type=F32)
        for b in range(blocks):
            block = product[:, b * pcols:(b + 1) * pcols]
            ref[slot, b] = (block + mine[0, b] if ready else block).astype(ref.dtype)

    cuts = [(b, r * half // 2, half // 2) for b in range(blocks) for r in range(4)]

    def part_of(ref, slot, i):
        b, r, count = cuts[i]
        return ref.at[slot, b, pl.ds(r, count)]

    def send_part(c, i, dst, slot, recv_sem, target):
        return pltpu.make_async_remote_copy(
            src_ref=part_of(parts, c, i), dst_ref=part_of(dst, slot, i),
            send_sem=p_send.at[c], recv_sem=recv_sem,
            device_id={"tp": target}, device_id_type=MESH,
        )

    def whole_part(c, slot):
        return pltpu.make_async_remote_copy(
            src_ref=parts.at[c], dst_ref=got.at[slot], send_sem=p_send.at[c], recv_sem=g_recv.at[slot],
            device_id={"tp": mt}, device_id_type=MESH,
        )

    def drain():
        if square:
            several(7, hop_recv.at[0]).wait_send()
        else:
            several(n - 1, hop_recv.at[0]).wait_send()

    pieces = len(cuts)
    early_pieces = pieces - 4

    def combined(i):
        return f_recv.at[max(i - early_pieces + 1, 0)]

    if line:
        m0, m1, m2, m3 = (mirror(d) for d in range(4))

        def send_product(c, t, dst, slot, recv_sems, target, ready=0):
            project(t, parts, c, ready)
            for i in range(pieces):
                send_part(c, i, dst, slot, recv_sems(i), target).start()

        def keep_own():
            project(mt, mine, 0)

        @pl.when(inner == 0)
        def _():
            send_product(0, m3, relay, 0, lambda i: r_recv.at[0, i], m1, done if early else 0)
            send_product(1, m2, relay, 1, lambda i: r_recv.at[1, i], m1)
            keep_own()

        @pl.when(jnp.logical_and(inner == 0, core == 0))
        def _():
            whole_part(1, 0).wait_send()

        @pl.when(inner == 0)
        def _():
            send_product(2, m1, got, 0, lambda i: g_recv.at[0], m1)

        @pl.when(inner == 1)
        def _():
            send_product(2, m0, got, 0, lambda i: g_recv.at[0], m0, done if early else 0)
            for c, t in ((1, m3), (2, m2), (0, mt)):
                project(t, mine, c)
            for c, target in ((0, m3), (1, m2)):
                for i in range(pieces):
                    b, r = cuts[i][0], pl.ds(*cuts[i][1:])
                    send_part(2, i, relay, c, r_recv.at[c, i], m0).wait_recv()
                    parts[c, b, r] = (mine[1 + c, b, r] + relay[c, b, r].astype(F32)).astype(BF16)
                    send_part(c, i, got, 1, combined(i), target).start()

        drain()
        whole_part(0, 0).wait_send()
        whole_part(2, 0).wait_recv()
        for b in range(blocks):
            mine[0, b] = mine[0, b] + got[0, b].astype(F32)
        @pl.when(jnp.logical_or(inner == 1, core == 1))
        def _():
            whole_part(1 + inner, 0).wait_send()

        if early_pieces:
            begun = pl.ds(0, blocks - 1)
            pltpu.make_async_remote_copy(
                src_ref=got.at[1, begun], dst_ref=got.at[1, begun], send_sem=p_send.at[0],
                recv_sem=combined(0), device_id={"tp": mt}, device_id_type=MESH,
            ).wait_recv()
        for i in range(pieces):
            b, r = cuts[i][0], pl.ds(*cuts[i][1:])
            if i >= early_pieces:
                send_part(2, i, got, 1, combined(i), m0).wait_recv()
            out_ref[r, b * pcols:(b + 1) * pcols] = (mine[0, b, r] + got[1, b, r].astype(F32)).astype(BF16)
        whole_part(2 - inner, 0).wait_send()
    else:
        ahead = sorted(range(1, tp), key=lambda j: -min(j, tp - j))
        for j in ahead:
            t = (mt + j) % tp
            project(t, parts, j)
            for i in range(pieces):
                send_part(j, i, got, mt, g_recv.at[mt], t).start()
        project(mt, mine, 0)
        drain()
        for j in reversed(ahead):
            source = (mt + j) % tp
            whole_part(j, source).wait_recv()
            for b in range(blocks):
                mine[0, b] = mine[0, b] + got[source, b].astype(F32)
        for b in range(blocks):
            out_ref[:, b * pcols:(b + 1) * pcols] = mine[0, b].astype(BF16)
        for j in ahead:
            whole_part(j, 0).wait_send()


def solution(mesh):
    n, tp = mesh.shape["seq"], mesh.shape["tp"]

    def per_device(queries, keyvalues, stretch_order, block_table, proj_weight):
        rows, q_width = queries.shape
        kv_heads = keyvalues.shape[2] // HEAD
        width = proj_weight.shape[1] // tp
        pcols = 2 * HEAD if width % (2 * HEAD) == 0 else HEAD
        blocks = width // pcols
        group_rows = q_width // HEAD // kv_heads * rows
        line = tp == 4
        n_parts, n_got, n_mine = (3, 2, 3) if line else (tp, tp, 1)
        dma = pltpu.SemaphoreType.DMA
        args = (queries, keyvalues, stretch_order, block_table, proj_weight)
        return pl.pallas_call(
            functools.partial(kernel, n, tp),
            out_shape=pltpu.VMEM((rows, width), BF16),
            in_specs=[pl.BlockSpec(memory_space=pltpu.HBM)] * 5,
            out_specs=pl.BlockSpec(memory_space=pltpu.VMEM),
            scratch_shapes=[
                pltpu.SMEM(stretch_order.shape, jnp.int32),
                pltpu.SMEM(block_table.shape, jnp.int32),
                pltpu.VMEM((rows, q_width), BF16),
                pltpu.VMEM((kv_heads, HEAD, group_rows), BF16),
                pltpu.VMEM((n, kv_heads, 2, rows, HEAD), BF16),
                pltpu.VMEM(proj_weight.shape, BF16),
                pltpu.VMEM((kv_heads, 1, group_rows), F32),
                pltpu.VMEM((kv_heads, HEAD, group_rows), F32),
                pltpu.VMEM((kv_heads, 8, group_rows), F32),
                pltpu.VMEM((rows, q_width), BF16),
                pltpu.VMEM((n_mine, blocks, rows, pcols), F32),
                pltpu.VMEM((n_parts, blocks, rows, pcols), BF16),
                pltpu.VMEM((2, blocks, rows, pcols), BF16),
                pltpu.VMEM((n_got, blocks, rows, pcols), BF16),
                dma((5,)), dma(()), dma((4 * kv_heads if n == 8 else n,)), dma((1 + 2 * kv_heads,)),
                dma((n_parts,)), dma((2, 4 * blocks)), dma((1 if line else tp,)), dma((5,)),
                pltpu.SemaphoreType.REGULAR,
            ],
            compiler_params=pltpu.CompilerParams(
                collective_id=0, has_side_effects=True, vmem_limit_bytes=48 << 20,
            ),
        )(*(pltpu.with_memory_space_constraint(a, pltpu.HBM) for a in args))

    return jax.shard_map(
        per_device, mesh=mesh,
        in_specs=(P("seq", "tp"), P(None, "seq", "tp"), P(), P(), P("tp", None)),
        out_specs=P("seq", "tp"), check_vma=False,
    )
```

```python
import functools

import jax
import jax.numpy as jnp
from jax import lax
from jax.experimental import pallas as pl
from jax.experimental.pallas import tpu as pltpu
from jax.sharding import PartitionSpec as P

HEAD = 128
MASKED = -1e30
LOG2E = 1.4426950408889634
MESH = pl.DeviceIdType.MESH
F32 = jnp.float32
BF16 = jnp.bfloat16


def kernel(
    n, tp, q_hbm, kv_hbm, order_hbm, table_hbm, w_hbm, out_ref,
    order, table, q_in, q_t, kv_buf, w_buf, top_ref, acc, den, att, mine, parts, relay, got,
    in_sem, kv_send, kv_recv, hop_recv, p_send, r_recv, g_recv, f_recv, go,
):
    rows = q_in.shape[0]
    kv_heads = kv_buf.shape[1]
    q_heads = q_in.shape[1] // HEAD
    group = q_heads // kv_heads
    width = out_ref.shape[1]
    blocks, _, pcols = parts.shape[1:]
    half = rows // 2
    chips = n // 2
    me = lax.axis_index("seq")
    mt = lax.axis_index("tp")
    chip = me // 2
    core = me % 2
    partner = chip * 2 + 1 - core
    heads = range(kv_heads)

    own = [
        pltpu.make_async_copy(
            kv_hbm.at[i, :, slice(g * HEAD, (g + 1) * HEAD)], kv_buf.at[me, g, i], in_sem.at[4]
        )
        for g in heads for i in range(2)
    ]
    load_q = pltpu.make_async_copy(q_hbm, q_in, in_sem.at[0])
    load_w = pltpu.make_async_copy(w_hbm, w_buf, in_sem.at[1])
    load_order = pltpu.make_async_copy(order_hbm, order, in_sem.at[2])
    load_table = pltpu.make_async_copy(table_hbm, table, in_sem.at[3])
    for c in own:
        c.start()
    load_q.start()
    load_order.start()
    load_table.start()
    load_w.start()

    barrier = pltpu.get_barrier_semaphore()

    def peer(j):
        return ((chip + j) % chips) * 2 + core

    def each(lo, hi, body):
        if hi - lo <= 8:
            for j in range(lo, hi):
                body(j)
        else:
            lax.fori_loop(lo, hi, lambda j, c: (body(j), c)[1], 0)

    def greet_seq(s):
        pl.semaphore_signal(barrier, inc=1, device_id={"seq": s}, device_id_type=MESH)

    def greet_tp(t):
        pl.semaphore_signal(barrier, inc=1, device_id={"tp": t}, device_id_type=MESH)

    square = chips == 4
    chip_x, chip_y = chip % 2, chip // 2
    x0 = (chip_y * 2 + 1 - chip_x) * 2
    y0 = ((1 - chip_y) * 2 + chip_x) * 2
    d0 = ((1 - chip_y) * 2 + 1 - chip_x) * 2
    x1, y1, d1 = x0 + 1, y0 + 1, d0 + 1
    line = tp == 4
    side = mt // 2
    inner = mt % 2 * (1 - side) + (1 - mt % 2) * side

    def mirror(d):
        return d * (1 - side) + (3 - d) * side

    def entered(t):
        pl.semaphore_signal(barrier, inc=1, device_id={"seq": chip * 2, "tp": t}, device_id_type=MESH)

    split = square and line
    if split:
        @pl.when(core == 0)
        def _():
            greet_seq(partner)

        greet_seq(x0 + core)
        greet_seq(y0 + core)
        entered(mirror(2))
        entered(mirror(1 - inner))

        @pl.when(inner == 1)
        def _():
            entered(mirror(3))

        def tell_partner():
            pl.semaphore_signal(go, inc=1, device_id={"seq": partner}, device_id_type=MESH)

        @pl.when(core == 1)
        def _():
            pl.semaphore_wait(barrier, 3)
            tell_partner()

        @pl.when(core == 0)
        def _():
            pl.semaphore_wait(go, 1)
    else:
        greet_seq(partner)
        if square:
            for s in (x0, x1, y0, y1):
                greet_seq(s)
            seq_peers = 5
        else:
            each(1, chips, lambda j: greet_seq(peer(j)))
            seq_peers = chips
        if line:
            greet_tp(mirror(2))
            greet_tp(mirror(1 - inner))

            @pl.when(inner == 1)
            def _():
                greet_tp(mirror(3))

            tp_peers = 2 + inner
        else:
            for j in range(1, tp):
                greet_tp((mt + j) % tp)
            tp_peers = tp - 1
        pl.semaphore_wait(barrier, seq_peers + tp_peers)

    pltpu.make_async_copy(kv_buf.at[me], kv_buf.at[me], in_sem.at[4]).wait()

    def copy(ref, recv_sem, target):
        return pltpu.make_async_remote_copy(
            src_ref=ref, dst_ref=ref, send_sem=kv_send, recv_sem=recv_sem,
            device_id={"seq": target}, device_id_type=MESH,
        )

    def slot(s, target):
        return copy(kv_buf.at[s], kv_recv.at[s], target)

    def relay_sem(axis, c, g):
        return kv_recv.at[(axis * 2 + c) * kv_heads + g]

    def near_sem(c, g):
        return kv_recv.at[c * kv_heads + g]

    def far_sem(c, g):
        return kv_recv.at[(2 + c) * kv_heads + g]

    def pair(recv_sem):
        return copy(kv_buf.at[0, 0], recv_sem, partner)

    def several(slots, recv_sem):
        return copy(kv_buf.at[pl.ds(0, slots)], recv_sem, partner)

    if square:

        for g in heads:
            copy(kv_buf.at[me, g, 0], relay_sem(0, core, g), x1).start()
            copy(kv_buf.at[me, g, 1], relay_sem(1, core, g), y1).start()
        for g in heads:
            for i in range(2):
                copy(kv_buf.at[me, g, i], hop_recv.at[0], partner).start()
    else:
        slot(me, partner).start()
        each(1, chips, lambda j: slot(me, peer(j)).start())

    load_q.wait()
    for g in heads:
        for j in range(group):
            h = g * group + j
            q_t[g, :, j * rows:(j + 1) * rows] = q_in[:, h * HEAD:(h + 1) * HEAD].T

    load_order.wait()
    load_table.wait()
    my_stretch = order[me]
    scale = LOG2E / HEAD**0.5

    def bias_of(s):
        key_stretch = order[s]
        seen = jnp.logical_and(key_stretch < my_stretch, table[my_stretch, key_stretch] == 1)
        return jnp.where(seen, 0.0, MASKED).astype(F32)

    def attend(g, slots, first=False):
        queries = q_t[g]
        scores, tops, biases = [], [], []
        for i, s in enumerate(slots):
            part = jnp.dot(kv_buf[s, g, 0], queries, preferred_element_type=F32)
            if first and i == 0:
                k_pos = lax.broadcasted_iota(jnp.int32, part.shape, 0)
                q_pos = lax.broadcasted_iota(jnp.int32, part.shape, 1) % rows
                part = jnp.where(k_pos <= q_pos, part, MASKED)
                bias = 0.0
            else:
                bias = bias_of(s)
            scores.append(part)
            biases.append(bias)
            tops.append(jnp.max(part, axis=0, keepdims=True) + bias)
        new_top = functools.reduce(jnp.maximum, tops)
        if not first:
            old_top = top_ref[g]
            new_top = jnp.maximum(new_top, old_top)
        weights = jnp.concatenate(
            [jnp.exp2((p - (new_top - b)) * scale).astype(BF16) for p, b in zip(scores, biases)], axis=0
        )
        values = jnp.concatenate([kv_buf[s, g, 1] for s in slots], axis=0).T
        tall = jnp.concatenate([values, jnp.ones((16, values.shape[1]), BF16)], axis=0)
        added = jnp.dot(tall, weights, preferred_element_type=F32)
        if first:
            acc[g] = added[:HEAD]
            den[g] = added[HEAD:HEAD + 8]
        else:
            fade = jnp.exp2((old_top - new_top) * scale)
            acc[g] = acc[g] * fade + added[:HEAD]
            den[g] = den[g] * fade + added[HEAD:HEAD + 8]
        top_ref[g] = new_top

    if split:
        @pl.when(core == 0)
        def _():
            pl.semaphore_wait(barrier, 2 + 2 * (2 + inner))
            tell_partner()

        @pl.when(core == 1)
        def _():
            pl.semaphore_wait(go, 1)

    def begin():
        for g in heads:
            attend(g, [me, partner], True)

    def normalise(g):
        share = 1.0 / den[g][0:1]
        for j in range(group):
            h = g * group + j
            cols = slice(j * rows, (j + 1) * rows)
            att[:, h * HEAD:(h + 1) * HEAD] = (acc[g, :, cols] * share[:, cols]).astype(BF16).T

    last = kv_heads - 1
    done = last * group * HEAD
    early = split and done > 0
    first_part = mirror(3) * (1 - inner) + mirror(0) * inner

    def columns(t):
        return pl.ds(pl.multiple_of(t * width, width), width)

    def look_ahead(g):
        if early and g == last:
            for k in range(last):
                normalise(k)
            ahead = jnp.dot(att[:, :done], w_buf[:done, columns(first_part)], preferred_element_type=F32)
            for b in range(blocks):
                mine[0, b] = ahead[:, b * pcols:(b + 1) * pcols]

    if square:
        for g in heads:
            copy(kv_buf.at[me, g, 1], near_sem(core, g), x0).start()
            copy(kv_buf.at[me, g, 0], near_sem(core, g), y0).start()
        near, far = [x1, y1, x0, y0], [d1, d0]

        def hand_over(s, g, i, hop):
            copy(kv_buf.at[s, g, i], hop_recv.at[hop], partner).start()

        @pl.when(core == 1)
        def _():
            for g in heads:
                for c, sx, sy in ((1, x1, y1), (0, x0, y0)):
                    for axis, s, target in ((0, sx, y0), (1, sy, x0)):
                        ref = kv_buf.at[s, g, axis]
                        copy(ref, relay_sem(axis, c, g), partner).wait_recv()
                        copy(ref, far_sem(c, g), target).start()
                        hand_over(s, g, axis, 1 + g)
            several(1, hop_recv.at[0]).wait_recv()
            begin()
            load_w.wait()
            for slots, hop in ((near, 1), (far, 1 + kv_heads)):
                for g in heads:
                    several(1, hop_recv.at[hop + g]).wait_recv()
                    if slots is far:
                        look_ahead(g)
                    attend(g, slots)

        @pl.when(core == 0)
        def _():
            several(1, hop_recv.at[0]).wait_recv()
            begin()
            load_w.wait()
            for g in heads:
                for c, sx, sy in ((1, x1, y1), (0, x0, y0)):
                    pair(near_sem(c, g)).wait_recv()
                    hand_over(sx, g, 1, 1 + g)
                    hand_over(sy, g, 0, 1 + g)
                several(1, hop_recv.at[1 + g]).wait_recv()
                attend(g, near)
            for g in heads:
                for c, s in ((1, d1), (0, d0)):
                    pair(far_sem(c, g)).wait_recv()
                    for i in range(2):
                        hand_over(s, g, i, 1 + kv_heads + g)
                look_ahead(g)
                attend(g, far)
    else:
        slot(partner, partner).wait_recv()
        begin()
        load_w.wait()

        def step(j):
            s = ((chip - j + chips) % chips) * 2 + core
            other = ((chip - j + chips) % chips) * 2 + 1 - core
            slot(s, partner).wait_recv()
            slot(s, partner).start()
            slot(other, partner).wait_recv()
            for g in heads:
                attend(g, [s, other])

        each(1, chips, step)

    for g in [last] if early else heads:
        normalise(g)

    def project(t, ref, slot, ready=0):
        product = jnp.dot(att[:, ready:], w_buf[ready:, columns(t)], preferred_element_type=F32)
        for b in range(blocks):
            block = product[:, b * pcols:(b + 1) * pcols]
            ref[slot, b] = (block + mine[0, b] if ready else block).astype(ref.dtype)

    cuts = [(b, r * half // 2, half // 2) for b in range(blocks) for r in range(4)]

    def part_of(ref, slot, i):
        b, r, count = cuts[i]
        return ref.at[slot, b, pl.ds(r, count)]

    def send_part(c, i, dst, slot, recv_sem, target):
        return pltpu.make_async_remote_copy(
            src_ref=part_of(parts, c, i), dst_ref=part_of(dst, slot, i),
            send_sem=p_send.at[c], recv_sem=recv_sem,
            device_id={"tp": target}, device_id_type=MESH,
        )

    def whole_part(c, slot):
        return pltpu.make_async_remote_copy(
            src_ref=parts.at[c], dst_ref=got.at[slot], send_sem=p_send.at[c], recv_sem=g_recv.at[slot],
            device_id={"tp": mt}, device_id_type=MESH,
        )

    def drain():
        if square:
            several(7, hop_recv.at[0]).wait_send()
        else:
            several(n - 1, hop_recv.at[0]).wait_send()

    pieces = len(cuts)
    early_pieces = pieces - 4

    def combined(i):
        return f_recv.at[max(i - early_pieces + 1, 0)]

    if line:
        m0, m1, m2, m3 = (mirror(d) for d in range(4))

        def send_product(c, t, dst, slot, recv_sems, target, ready=0):
            project(t, parts, c, ready)
            for i in range(pieces):
                send_part(c, i, dst, slot, recv_sems(i), target).start()

        def keep_own():
            project(mt, mine, 0)

        @pl.when(inner == 0)
        def _():
            send_product(0, m3, relay, 0, lambda i: r_recv.at[0, i], m1, done if early else 0)
            send_product(1, m2, relay, 1, lambda i: r_recv.at[1, i], m1)
            keep_own()

        @pl.when(inner == 0)
        def _():
            send_product(2, m1, got, 0, lambda i: g_recv.at[0], m1)

        @pl.when(inner == 1)
        def _():
            send_product(2, m0, got, 0, lambda i: g_recv.at[0], m0, done if early else 0)
            for c, t in ((1, m3), (2, m2), (0, mt)):
                project(t, mine, c)
            for c, target in ((0, m3), (1, m2)):
                for i in range(pieces):
                    b, r = cuts[i][0], pl.ds(*cuts[i][1:])
                    send_part(2, i, relay, c, r_recv.at[c, i], m0).wait_recv()
                    parts[c, b, r] = (mine[1 + c, b, r] + relay[c, b, r].astype(F32)).astype(BF16)
                    send_part(c, i, got, 1, combined(i), target).start()

        drain()
        whole_part(0, 0).wait_send()
        whole_part(2, 0).wait_recv()
        for b in range(blocks):
            mine[0, b] = mine[0, b] + got[0, b].astype(F32)
        whole_part(1 + inner, 0).wait_send()

        if early_pieces:
            begun = pl.ds(0, blocks - 1)
            pltpu.make_async_remote_copy(
                src_ref=got.at[1, begun], dst_ref=got.at[1, begun], send_sem=p_send.at[0],
                recv_sem=combined(0), device_id={"tp": mt}, device_id_type=MESH,
            ).wait_recv()
        for i in range(pieces):
            b, r = cuts[i][0], pl.ds(*cuts[i][1:])
            if i >= early_pieces:
                send_part(2, i, got, 1, combined(i), m0).wait_recv()
            out_ref[r, b * pcols:(b + 1) * pcols] = (mine[0, b, r] + got[1, b, r].astype(F32)).astype(BF16)
        whole_part(2 - inner, 0).wait_send()
    else:
        ahead = sorted(range(1, tp), key=lambda j: -min(j, tp - j))
        for j in ahead:
            t = (mt + j) % tp
            project(t, parts, j)
            for i in range(pieces):
                send_part(j, i, got, mt, g_recv.at[mt], t).start()
        project(mt, mine, 0)
        drain()
        for j in reversed(ahead):
            source = (mt + j) % tp
            whole_part(j, source).wait_recv()
            for b in range(blocks):
                mine[0, b] = mine[0, b] + got[source, b].astype(F32)
        for b in range(blocks):
            out_ref[:, b * pcols:(b + 1) * pcols] = mine[0, b].astype(BF16)
        for j in ahead:
            whole_part(j, 0).wait_send()


def solution(mesh):
    n, tp = mesh.shape["seq"], mesh.shape["tp"]

    def per_device(queries, keyvalues, stretch_order, block_table, proj_weight):
        rows, q_width = queries.shape
        kv_heads = keyvalues.shape[2] // HEAD
        width = proj_weight.shape[1] // tp
        pcols = 2 * HEAD if width % (2 * HEAD) == 0 else HEAD
        blocks = width // pcols
        group_rows = q_width // HEAD // kv_heads * rows
        line = tp == 4
        n_parts, n_got, n_mine = (3, 2, 3) if line else (tp, tp, 1)
        dma = pltpu.SemaphoreType.DMA
        args = (queries, keyvalues, stretch_order, block_table, proj_weight)
        return pl.pallas_call(
            functools.partial(kernel, n, tp),
            out_shape=pltpu.VMEM((rows, width), BF16),
            in_specs=[pl.BlockSpec(memory_space=pltpu.HBM)] * 5,
            out_specs=pl.BlockSpec(memory_space=pltpu.VMEM),
            scratch_shapes=[
                pltpu.SMEM(stretch_order.shape, jnp.int32),
                pltpu.SMEM(block_table.shape, jnp.int32),
                pltpu.VMEM((rows, q_width), BF16),
                pltpu.VMEM((kv_heads, HEAD, group_rows), BF16),
                pltpu.VMEM((n, kv_heads, 2, rows, HEAD), BF16),
                pltpu.VMEM(proj_weight.shape, BF16),
                pltpu.VMEM((kv_heads, 1, group_rows), F32),
                pltpu.VMEM((kv_heads, HEAD, group_rows), F32),
                pltpu.VMEM((kv_heads, 8, group_rows), F32),
                pltpu.VMEM((rows, q_width), BF16),
                pltpu.VMEM((n_mine, blocks, rows, pcols), F32),
                pltpu.VMEM((n_parts, blocks, rows, pcols), BF16),
                pltpu.VMEM((2, blocks, rows, pcols), BF16),
                pltpu.VMEM((n_got, blocks, rows, pcols), BF16),
                dma((5,)), dma(()), dma((4 * kv_heads if n == 8 else n,)), dma((1 + 2 * kv_heads,)),
                dma((n_parts,)), dma((2, 4 * blocks)), dma((1 if line else tp,)), dma((5,)),
                pltpu.SemaphoreType.REGULAR,
            ],
            compiler_params=pltpu.CompilerParams(
                collective_id=0, has_side_effects=True, vmem_limit_bytes=48 << 20,
            ),
        )(*(pltpu.with_memory_space_constraint(a, pltpu.HBM) for a in args))

    return jax.shard_map(
        per_device, mesh=mesh,
        in_specs=(P("seq", "tp"), P(None, "seq", "tp"), P(), P(), P("tp", None)),
        out_specs=P("seq", "tp"), check_vma=False,
    )
```
